256 devices in a mesh: grp: 2 (over y), seq: 128 (over z, x, core).
Axes of the slice: x: 4, y: 2, z: 16, core: 2. Of those that a mesh axis runs over, the one named last changes fastest.
The devices are a block of a 4x16x16 slice.
Arguments:
- frames: bfloat16 [4, 81920, 1280], P('grp', 'seq'), parts along dimension 0, may hold values from -120 to 120
- dec_states: bfloat16 [2, 256, 1280], P(None, 'grp'), parts along dimension 1, may hold values from -6 to 6
- w_query: bfloat16 [1280, 1280], P(None, 'seq'), may hold values from -0.15625 to 0.15625
- w_keyval: bfloat16 [1280, 2560], replicated, may hold values from -0.15625 to 0.15625
- w_output: bfloat16 [1280, 1280], P(None, 'seq'), may hold values from -0.15625 to 0.15625
- head_slope: float32 [20], replicated, may hold values from 0.3 to 12
- lengths: int32 [4, 128], P('grp'), parts along dimension 0, may hold values from 128 to 640, as said below
- positions: int32 [2, 256], P(None, 'grp'), parts along dimension 1, may hold values from 0 to 127
Outputs:
- attended: bfloat16 [2, 256, 1280], P(None, 'grp', 'seq'), parts along dimension 1
The draws below stay inside these ranges and needn't reach their ends.
There are 2 independent parts, one for each index of `grp`. The reference program is written for one: setup_inputs(seed, part) draws one part's arguments, and reference() takes and returns one part's arrays. A program takes and returns all parts, laid end to end along the dimension named above; an argument that names none is the same for every part. Nothing has to cross between parts.
Inputs may be any that keep to these rules, and one draw needn't show every extreme that they name: `lengths`: every step has one block of exactly 640 valid frames.
All inputs are finite; a program needn't handle non-finite values.
Results may differ from the reference program's by a relative error of at most 0.005.
The reference program's roundings to bfloat16 on the way count: a program that leaves them out, or rounds other values in their place, can miss the bound.
Values may be sent and summed in bfloat16 or wider, within the bound.
No kernel may reach another device: no remote copies, remote signals or barrier semaphores. Data moves between devices by JAX's collectives and lax.ppermute only.
A program may use at most 128 MiB of HBM per device.

```python
import math
import jax
import jax.numpy as jnp
from jax import lax

D = 1280
H = 20
FR = 640
STEPS = 2
QROWS = 128
N_SEQ = 128


def draw_frames(key, part):
    key_base = jax.random.fold_in(key, 11)
    base = jax.random.normal(key_base, (STEPS, N_SEQ * FR, D), jnp.float32)
    base = jnp.clip(base, -6.0, 6.0)
    return base.astype(jnp.bfloat16)


def draw_lengths(key, part):
    key_pick = jax.random.fold_in(key, 21)
    key_long = jax.random.fold_in(key, 22)
    lowest = FR // 5
    spread = FR - lowest
    picked = jax.random.randint(key_pick, (STEPS, N_SEQ), 0, spread + 1)
    frame_counts = lowest + picked * picked // spread
    longest = jax.random.randint(key_long, (STEPS,), 0, N_SEQ)
    longest_at = jnp.arange(N_SEQ, dtype=jnp.int32)[None, :] == longest[:, None]
    return jnp.where(longest_at, FR, frame_counts).astype(jnp.int32)


def plant(values, own_key, smallest, high):
    spot = [jax.random.randint(jax.random.fold_in(own_key, axis), (), 0, length) for axis, length in enumerate(values.shape)]
    main_axis = values.shape.index(max(values.shape))
    neighbour = spot[:main_axis] + [(spot[main_axis] + 1) % values.shape[main_axis]] + spot[main_axis + 1:]
    return values.at[tuple(spot)].set(smallest).at[tuple(neighbour)].set(high)


def block_levels(own_key, extent, split, least, largest):
    level, own = 1.0, jax.random.fold_in(own_key, 6)
    for axis_at, shards_of in split:
        draws = jnp.exp(jax.random.uniform(jax.random.fold_in(own, axis_at), (shards_of,), jnp.float32, least / len(split), largest / len(split)))
        level = level * jnp.repeat(draws, extent[axis_at] // shards_of).reshape([-1 if axis == axis_at else 1 for axis in range(len(extent))])
    return level


def noise(rng, shape, scale, most, pieces=(), kind=jnp.bfloat16):
    result = jax.random.normal(rng, shape, jnp.float32) * scale
    if len(pieces) > 0:
        result = block_levels(rng, shape, pieces, -0.22, 0.18) * result
    return jnp.clip(result, min=-most, max=most).astype(kind)


def setup_inputs(seed: int = 0, part: int = 0) -> dict:
    splits = jax.random.split(jax.random.key(seed), 9)
    part_splits = jax.random.split(jax.random.fold_in(splits[8], part), 9)
    return {
        "frames": draw_frames(jax.random.fold_in(jax.random.fold_in(splits[8], part), 71), part),
        "dec_states": noise(part_splits[1], (STEPS, QROWS, D), 1.0, 6.0),
        "w_query": noise(splits[2], (D, D), D ** -0.5, 0.15625, ((1, 128),)),
        "w_keyval": noise(splits[3], (D, 2 * D), D ** -0.5, 0.15625),
        "w_output": noise(splits[4], (D, D), D ** -0.5, 0.15625, ((1, 128),)),
        "head_slope": jnp.clip(jnp.exp(jax.random.uniform(splits[5], (H,), jnp.float32, math.log(0.3), math.log(12.0))), 0.3, 12.0),
        "lengths": draw_lengths(jax.random.fold_in(jax.random.fold_in(splits[8], part), 71), part),
        "positions": plant(jax.random.randint(part_splits[7], (STEPS, QROWS), 0, N_SEQ), jax.random.fold_in(part_splits[7], 1), 0, N_SEQ - 1).astype(jnp.int32),
    }


def reference(frames, dec_states, w_query, w_keyval, w_output, head_slope, lengths, positions):
    step_count, total_frames, model_width = frames.shape
    query_rows = dec_states.shape[1]
    head_count = head_slope.shape[0]
    head_size = model_width // head_count
    block_count = N_SEQ
    frame_count = total_frames // block_count
    keyval = jnp.dot(frames.reshape(step_count * total_frames, model_width), w_keyval, preferred_element_type=jnp.float32).astype(jnp.bfloat16)
    all_keys = keyval[:, :model_width].reshape(step_count, block_count, frame_count, head_count, head_size)
    all_values = keyval[:, model_width:].reshape(step_count, block_count, frame_count, head_count, head_size)
    queries = jnp.dot(dec_states.reshape(step_count * query_rows, model_width), w_query, preferred_element_type=jnp.float32).astype(jnp.bfloat16)
    queries = queries.reshape(step_count, query_rows, head_count, head_size)
    results = []
    for step_now in range(step_count):
        query_now = queries[step_now].astype(jnp.float32)
        row_positions = positions[step_now].astype(jnp.float32)

        def one_block(flat_index):
            older_step = flat_index // block_count
            block_index = flat_index % block_count
            block_keys = all_keys[older_step, block_index].astype(jnp.float32)
            block_values = all_values[older_step, block_index].astype(jnp.float32)
            scores = jnp.einsum('qhd,jhd->hqj', query_now, block_keys) / math.sqrt(head_size)
            slot_place = ((block_index + 1) % block_count).astype(jnp.float32)
            age_steps = (step_now - older_step).astype(jnp.float32)
            distance = jnp.abs(row_positions - slot_place) / block_count + age_steps
            scores = scores - head_slope[:, None, None] * distance[None, :, None]
            length_now = lengths[older_step, block_index]
            valid = jnp.arange(frame_count, dtype=jnp.int32)[None, None, :] < length_now
            scores = jnp.where(valid, scores, -jnp.inf)
            row_peak = lax.optimization_barrier(jnp.max(scores, axis=2))
            weights = jnp.exp(scores - row_peak[:, :, None]).astype(jnp.bfloat16).astype(jnp.float32)
            row_total = lax.optimization_barrier(jnp.sum(weights, axis=2))
            row_context = jnp.einsum('hqj,jhd->hqd', weights, block_values)
            return (row_peak, row_total, row_context)
        peaks, totals, contexts = lax.map(one_block, jnp.arange((step_now + 1) * block_count, dtype=jnp.int32))
        row_top = lax.optimization_barrier(jnp.max(peaks, axis=0))
        factors = jnp.exp(peaks - row_top[None])
        row_total = lax.optimization_barrier(jnp.sum(factors * totals, axis=0))
        row_context = lax.optimization_barrier(jnp.sum(factors[..., None] * contexts, axis=0))
        context = (row_context / row_total[..., None]).transpose(1, 0, 2).reshape(query_rows, model_width)
        context = context.astype(jnp.bfloat16)
        results.append(jnp.dot(context, w_output, preferred_element_type=jnp.float32).astype(jnp.bfloat16))
    return jnp.stack(results)
```

```python
import functools
import math

import jax
import jax.numpy as jnp
from jax import lax
from jax.experimental import pallas as pl
from jax.experimental.pallas import tpu as pltpu
from jax.sharding import Mesh
from jax.sharding import PartitionSpec as P

SEQ = ("seq_0", "seq_1", "seq_2")
BF16 = jnp.bfloat16
F32 = jnp.float32
SLAB = 32
PEAK_ROWS = 3
STAT_ROWS = 5
LOG2E = math.log2(math.e)


def split_rows(x, count):
    rows = []
    for _ in range(count):
        part = x.astype(BF16).astype(F32)
        rows.append(part)
        x = x - part
    return rows


def stat_rows(peak, total):
    return split_rows(peak, PEAK_ROWS) + split_rows(total, STAT_ROWS - PEAK_ROWS)


def attend_kernel(
    lengths_ref, slope_ref, q_ref, k_ref, vt_ref, dist_ref, msg_ref, stat_ref, *, frame_count, chunks
):
    pair = pl.program_id(0)
    head_size = q_ref.shape[0] // 2
    tokens = q_ref.shape[1]
    half = tokens // 2
    scale = 1.0 / math.sqrt(head_size)
    lanes = 2 * head_size

    def keys_of(block):
        keys = k_ref[block * frame_count : (block + 1) * frame_count, :]
        row = lax.broadcasted_iota(jnp.int32, (frame_count, lanes), 0)
        lane = lax.broadcasted_iota(jnp.int32, (frame_count, lanes), 1)
        invalid = jnp.logical_and(row >= lengths_ref[block], lane == 0)
        return jnp.concatenate([keys, jnp.where(invalid, 1.0, 0.0).astype(BF16)], axis=1)

    floor_row = lax.broadcasted_iota(jnp.int32, (lanes, tokens), 0)
    floor = jnp.where(floor_row == 0, -1e30, 0.0).astype(BF16)

    def weigh(keys, right):
        scores = jnp.dot(keys, right, preferred_element_type=F32)
        peak = jnp.max(scores, axis=0, keepdims=True)
        weights = jnp.exp2((scores - peak) * (scale * LOG2E)).astype(BF16)
        return peak * scale, weights

    ones = jnp.ones((16, frame_count), BF16)
    zeros = jnp.zeros((head_size, tokens), BF16)
    zeros_half = jnp.zeros((head_size, half), BF16)
    right = jnp.concatenate(
        [
            jnp.concatenate([q_ref[:head_size, half:], zeros_half], axis=1),
            jnp.concatenate([zeros_half, q_ref[head_size:, half:]], axis=1),
            floor,
        ],
        axis=0,
    )
    new_peak, new_weights = weigh(keys_of(1), right)
    new_sum = jnp.dot(
        jnp.concatenate([vt_ref[:, frame_count:], ones], axis=0),
        new_weights,
        preferred_element_type=F32,
    )
    old_keys = keys_of(0)
    for side in range(2):
        head = 2 * pair + side
        own = q_ref[side * head_size : (side + 1) * head_size, :]
        right = jnp.concatenate([own, zeros, floor] if side == 0 else [zeros, own, floor], axis=0)
        old_peak, old_weights = weigh(old_keys, right)
        old_sum = jnp.dot(
            jnp.concatenate(
                [vt_ref[side * head_size : (side + 1) * head_size, :frame_count], ones], axis=0
            ),
            old_weights,
            preferred_element_type=F32,
        )
        slope = slope_ref[head]
        old_peak = old_peak - slope * dist_ref[0:1, :]
        late_peak = new_peak[:, side * half : (side + 1) * half] - slope * dist_ref[1:2, half:]
        late = slice(side * half, (side + 1) * half)
        top = jnp.maximum(old_peak[:, half:], late_peak)
        old_factor = jnp.exp(old_peak[:, half:] - top)
        new_factor = jnp.exp(late_peak - top)
        old_total = old_sum[head_size : head_size + 1, :]
        new_total = new_sum[2 * head_size : 2 * head_size + 1, late]
        second = (
            old_sum[:head_size, half:] * old_factor
            + new_sum[side * head_size : (side + 1) * head_size, late] * new_factor
        )
        context = jnp.concatenate([old_sum[:head_size, :half], second], axis=1).astype(BF16)
        for part in range(head_size // SLAB):
            slab = head * (head_size // SLAB) + part
            chunk_slabs = (msg_ref.shape[1] - 16) // SLAB
            place = pl.multiple_of((slab % chunk_slabs) * SLAB, SLAB)
            msg_ref[slab // chunk_slabs, pl.ds(place, SLAB), :] = context[
                part * SLAB : (part + 1) * SLAB, :
            ]
        stat_ref[head, 0:1, :] = jnp.concatenate([old_peak[:, :half], top], axis=1)
        stat_ref[head, 1:2, :] = jnp.concatenate(
            [old_total[:, :half], old_total[:, half:] * old_factor + new_total * new_factor], axis=1
        )

    @pl.when(pair == pl.num_programs(0) - 1)
    def _():
        heads = stat_ref.shape[0]
        chunk_rows = msg_ref.shape[1] - 16
        for chunk in range(chunks):
            first = chunk * chunk_rows // head_size
            rows = []
            for head in range(first, first + 3):
                rows += stat_rows(stat_ref[head, 0:1, :], stat_ref[head, 1:2, :])
            rows.append(jnp.zeros_like(rows[0]))
            msg_ref[chunk, chunk_rows:, :] = jnp.concatenate(rows, axis=0).astype(BF16)


def attend(lengths, slope, queries, keys, values_t, dist, frame_count, chunks):
    width, tokens = queries.shape
    head_count = slope.shape[0]
    pair_rows = 2 * (width // head_count)
    rows = keys.shape[0]
    return pl.pallas_call(
        functools.partial(attend_kernel, frame_count=frame_count, chunks=chunks),
        grid=(head_count // 2,),
        in_specs=[
            pl.BlockSpec(memory_space=pltpu.SMEM),
            pl.BlockSpec(memory_space=pltpu.SMEM),
            pl.BlockSpec((pair_rows, tokens), lambda p: (p, 0)),
            pl.BlockSpec((rows, pair_rows), lambda p: (0, p)),
            pl.BlockSpec((pair_rows, rows), lambda p: (p, 0)),
            pl.BlockSpec(dist.shape, lambda p: (0, 0)),
        ],
        out_specs=pl.BlockSpec((chunks, width // chunks + 16, tokens), lambda p: (0, 0, 0)),
        out_shape=jax.ShapeDtypeStruct((chunks, width // chunks + 16, tokens), BF16),
        scratch_shapes=[pltpu.VMEM((head_count, 8, tokens), F32)],
        compiler_params=pltpu.CompilerParams(vmem_limit_bytes=40 << 20),
        name="attend",
    )(lengths, slope, queries, keys, values_t, dist)


def merge_kernel(odd_ref, in_ref, out_ref):
    sources, rows, tokens = in_ref.shape
    chunk_rows = rows - 16
    stats = [in_ref[:, chunk_rows + r, :].astype(F32) for r in range(3 * STAT_ROWS)]
    tops, totals, factors = [], [], []
    for slot in range(3):
        at = slot * STAT_ROWS
        peak = (stats[at] + stats[at + 1]) + stats[at + 2]
        top = jnp.max(peak, axis=0, keepdims=True)
        factor = jnp.exp(peak - top)
        tops.append(top)
        factors.append(factor)
        totals.append(jnp.sum(factor * (stats[at + 3] + stats[at + 4]), axis=0, keepdims=True))
    odd = odd_ref[0] == 1
    slabs, slab_stats = [], []
    for slab in range(chunk_rows // SLAB):
        even_slot, odd_slot = slab // 2, (slab + 1) // 2
        pick = lambda x: x[even_slot] if even_slot == odd_slot else jnp.where(odd, x[odd_slot], x[even_slot])
        factor = pick(factors)
        total = None
        for source in range(sources):
            part = in_ref[source, slab * SLAB : (slab + 1) * SLAB, :].astype(F32)
            part = part * factor[source : source + 1, :]
            total = part if total is None else total + part
        slabs.append(total)
        slab_stats.append(stat_rows(pick(tops), pick(totals)))
    merged = jnp.concatenate(slabs, axis=0)
    targets, out_rows, lanes = out_ref.shape
    pieces = targets // 2
    piece = chunk_rows // pieces
    for target in range(targets):
        side, at = target // pieces, (target % pieces) * piece
        cut = slice(side * lanes, (side + 1) * lanes)
        rows = slab_stats[at // SLAB] + slab_stats[(at + piece - 1) // SLAB]
        rows = [r[:, cut] for r in rows]
        rows.append(jnp.zeros((out_rows - piece - len(rows), lanes), F32))
        out_ref[target] = jnp.concatenate([merged[at : at + piece, cut]] + rows, axis=0).astype(BF16)


def finish_kernel(bound_ref, in_ref, out_ref, *, piece):
    sources, rows, lanes = in_ref.shape
    stats = [in_ref[:, piece + r, :].astype(F32) for r in range(2 * STAT_ROWS)]
    factors, totals = [], []
    for at in (0, STAT_ROWS):
        peak = (stats[at] + stats[at + 1]) + stats[at + 2]
        factor = jnp.exp(peak - jnp.max(peak, axis=0, keepdims=True))
        factors.append(factor)
        totals.append(jnp.sum(factor * (stats[at + 3] + stats[at + 4]), axis=0, keepdims=True))
    out_rows = out_ref.shape[0]
    row = lax.broadcasted_iota(jnp.int32, (out_rows, lanes), 0)
    first = row < bound_ref[0]
    total = None
    for source in range(sources):
        factor = jnp.where(first, factors[0][source : source + 1, :], factors[1][source : source + 1, :])
        part = in_ref[source, :out_rows, :].astype(F32) * factor
        total = part if total is None else total + part
    context = total / jnp.where(first, totals[0], totals[1])
    out_ref[...] = jnp.where(row < piece, context, 0.0).astype(BF16)


def project_kernel(ctx_ref, w_ref, out_ref):
    pieces, sides = ctx_ref.shape[:2]
    for side in range(sides):
        total = None
        for at in range(pieces):
            part = lax.dot_general(
                ctx_ref[at, side], w_ref[at], (((0,), (0,)), ((), ())), preferred_element_type=F32
            )
            total = part if total is None else total + part
        out_ref[side] = total.astype(BF16)


def whole(kernel, out_shape, scalars, arrays, name):
    return pl.pallas_call(
        kernel,
        in_specs=[pl.BlockSpec(memory_space=pltpu.SMEM)] * len(scalars)
        + [pl.BlockSpec(memory_space=pltpu.VMEM)] * len(arrays),
        out_specs=pl.BlockSpec(memory_space=pltpu.VMEM),
        out_shape=out_shape,
        compiler_params=pltpu.CompilerParams(vmem_limit_bytes=32 << 20),
        name=name,
    )(*scalars, *arrays)


def spread(x, axis):
    copies = jnp.broadcast_to(x[None], (lax.axis_size(axis), *x.shape))
    copies = lax.optimization_barrier(copies)
    return lax.all_to_all(copies, axis, 0, 0)


def local(frames, dec_states, w_query, w_keyval, w_output, head_slope, lengths, positions):
    devices = lax.axis_size(SEQ)
    own_index = lax.axis_index(SEQ)
    across, beside, cores = (lax.axis_size(axis) for axis in SEQ)
    step_count, frame_count, width = frames.shape
    query_rows = dec_states.shape[1]
    tokens = step_count * query_rows
    columns = w_query.shape[1]
    near = beside * cores

    own_queries = lax.dot_general(
        w_query,
        dec_states.reshape(tokens, width),
        (((0,), (1,)), ((), ())),
        preferred_element_type=F32,
    ).astype(BF16)
    padded = jnp.pad(own_queries, ((0, 16 - columns), (0, 0)))
    queries = spread(padded, "seq_0")[:, :columns]
    queries = spread(queries.reshape(across * columns, tokens), "seq_1")
    queries = lax.all_gather(queries, "seq_2")
    queries = queries.reshape(cores, beside, across, columns, tokens)
    queries = queries.transpose(2, 1, 0, 3, 4).reshape(width, tokens)

    frame_rows = frames.reshape(step_count * frame_count, width)
    keys = jnp.dot(frame_rows, w_keyval[:, :width], preferred_element_type=F32).astype(BF16)
    values_t = lax.dot_general(
        w_keyval[:, width:], frame_rows, (((0,), (1,)), ((), ())), preferred_element_type=F32
    ).astype(BF16)

    slot_place = ((own_index + 1) % devices).astype(F32)
    apart = jnp.abs(positions.astype(F32) - slot_place) / devices
    age = jnp.arange(step_count, dtype=F32)[:, None]
    dist = jnp.stack([(apart + age).reshape(tokens), apart.reshape(tokens)])
    dist = jnp.pad(dist, ((0, 6), (0, 0)))
    own_lengths = lax.dynamic_slice(lengths, (0, own_index), (step_count, 1)).reshape(step_count)

    message = attend(own_lengths, head_slope, queries, keys, values_t, dist, frame_count, near)
    message = lax.all_to_all(message, ("seq_1", "seq_2"), 0, 0)
    odd = (lax.axis_index(("seq_1", "seq_2")) % 2).astype(jnp.int32).reshape(1)
    piece = 2 * width // devices
    message = whole(
        merge_kernel,
        jax.ShapeDtypeStruct((across, SLAB, tokens // 2), BF16),
        [odd],
        [message],
        "merge",
    )
    message = lax.all_to_all(message, "seq_0", 0, 0)
    at = (lax.axis_index("seq_0") % (across // 2)) * piece
    bound = (SLAB - at % SLAB).astype(jnp.int32).reshape(1)
    context = whole(
        functools.partial(finish_kernel, piece=piece),
        jax.ShapeDtypeStruct((24, tokens // 2), BF16),
        [bound],
        [message],
        "finish",
    )
    context = spread(context, "seq_0")
    context = spread(context.reshape(across * 24, tokens // 2), "seq_1")
    context = lax.all_gather(context, "seq_2")
    context = context.reshape(near, 2, across // 2 * 24, tokens // 2)
    weights = w_output.reshape(beside, cores, across // 2, piece, columns)
    weights = jnp.pad(weights, ((0, 0), (0, 0), (0, 0), (0, 24 - piece), (0, 0)))
    weights = weights.transpose(1, 0, 2, 3, 4).reshape(near, across // 2 * 24, columns)
    return whole(
        project_kernel,
        jax.ShapeDtypeStruct((step_count, query_rows, columns), BF16),
        [],
        [context, weights],
        "project",
    )


def solution(mesh):
    finer = Mesh(
        mesh.devices.reshape(mesh.shape["grp"], 16, 4, 2), ("grp", "seq_0", "seq_1", "seq_2")
    )
    return jax.shard_map(
        local,
        mesh=finer,
        in_specs=(
            P("grp", SEQ, None),
            P(None, "grp", None),
            P(None, SEQ),
            P(),
            P(None, SEQ),
            P(),
            P("grp", None),
            P(None, "grp"),
        ),
        out_specs=P(None, "grp", SEQ),
        check_vma=False,
    )
```

```python
import functools
import math

import jax
import jax.numpy as jnp
from jax import lax
from jax.experimental import pallas as pl
from jax.experimental.pallas import tpu as pltpu
from jax.sharding import Mesh
from jax.sharding import PartitionSpec as P

SEQ = ("seq_0", "seq_1", "seq_2")
BF16 = jnp.bfloat16
F32 = jnp.float32
SLAB = 32
PEAK_ROWS = 3
STAT_ROWS = 5
LOG2E = math.log2(math.e)


def split_rows(x, count):
    rows = []
    for _ in range(count):
        part = x.astype(BF16).astype(F32)
        rows.append(part)
        x = x - part
    return rows


def stat_rows(peak, total):
    return split_rows(peak, PEAK_ROWS) + split_rows(total, STAT_ROWS - PEAK_ROWS)


def floor_div(x, n):
    return (x * (2**19 // n + 1)) >> 19


def pair_queries(pair, gathered_ref, rows, columns, beside):
    near, held, _ = gathered_ref.shape
    cores = near // beside
    window = 48
    span = near * columns
    first = jnp.minimum((pair * rows // span) * columns // 16, (held - window) // 16)
    start = pl.multiple_of(first * 16, 16)
    pieces = [gathered_ref[at, pl.ds(start, window), :] for at in range(near)]
    shape = (rows, near * window)
    at = pair * rows + lax.broadcasted_iota(jnp.int32, (rows, 128), 0)
    far = floor_div(at, span)
    rest = at - far * span
    owner = floor_div(rest, columns)
    column = rest - owner * columns
    core = owner & (cores - 1)
    source = core * beside + floor_div(owner, cores)
    source = source * window + far * columns + column - first * 16
    source = jnp.concatenate([source] * (near * window // 128), axis=1)
    picked = (lax.broadcasted_iota(jnp.int32, shape, 1) == source).astype(F32).astype(BF16)
    queries = jnp.dot(picked, jnp.concatenate(pieces, axis=0), preferred_element_type=F32)
    return queries.astype(BF16)


def attend_kernel(
    lengths_ref,
    slope_ref,
    gathered_ref,
    k_ref,
    vt_ref,
    dist_ref,
    msg_ref,
    stat_ref,
    *,
    frame_count,
    chunks,
    columns,
    beside,
):
    pair = pl.program_id(0)
    head_size = k_ref.shape[1] // 2
    tokens = gathered_ref.shape[2]
    queries = pair_queries(pair, gathered_ref, 2 * head_size, columns, beside)
    half = tokens // 2
    scale = 1.0 / math.sqrt(head_size)
    lanes = 2 * head_size

    def keys_of(block):
        keys = k_ref[block * frame_count : (block + 1) * frame_count, :]
        row = lax.broadcasted_iota(jnp.int32, (frame_count, lanes), 0)
        lane = lax.broadcasted_iota(jnp.int32, (frame_count, lanes), 1)
        invalid = jnp.logical_and(row >= lengths_ref[block], lane == 0)
        return jnp.concatenate([keys, jnp.where(invalid, 1.0, 0.0).astype(BF16)], axis=1)

    floor_row = lax.broadcasted_iota(jnp.int32, (lanes, tokens), 0)
    floor = jnp.where(floor_row == 0, -1e30, 0.0).astype(BF16)

    def weigh(keys, right):
        scores = jnp.dot(keys, right, preferred_element_type=F32)
        peak = jnp.max(scores, axis=0, keepdims=True)
        weights = jnp.exp2((scores - peak) * (scale * LOG2E)).astype(BF16)
        return peak * scale, weights

    ones = jnp.ones((16, frame_count), BF16)
    zeros = jnp.zeros((head_size, tokens), BF16)
    zeros_half = jnp.zeros((head_size, half), BF16)
    right = jnp.concatenate(
        [
            jnp.concatenate([queries[:head_size, half:], zeros_half], axis=1),
            jnp.concatenate([zeros_half, queries[head_size:, half:]], axis=1),
            floor,
        ],
        axis=0,
    )
    new_peak, new_weights = weigh(keys_of(1), right)
    new_sum = jnp.dot(
        jnp.concatenate([vt_ref[:, frame_count:], ones], axis=0),
        new_weights,
        preferred_element_type=F32,
    )
    old_keys = keys_of(0)
    for side in range(2):
        head = 2 * pair + side
        own = queries[side * head_size : (side + 1) * head_size, :]
        right = jnp.concatenate([own, zeros, floor] if side == 0 else [zeros, own, floor], axis=0)
        old_peak, old_weights = weigh(old_keys, right)
        old_sum = jnp.dot(
            jnp.concatenate(
                [vt_ref[side * head_size : (side + 1) * head_size, :frame_count], ones], axis=0
            ),
            old_weights,
            preferred_element_type=F32,
        )
        slope = slope_ref[head]
        old_peak = old_peak - slope * dist_ref[0:1, :]
        late_peak = new_peak[:, side * half : (side + 1) * half] - slope * dist_ref[1:2, half:]
        late = slice(side * half, (side + 1) * half)
        top = jnp.maximum(old_peak[:, half:], late_peak)
        old_factor = jnp.exp(old_peak[:, half:] - top)
        new_factor = jnp.exp(late_peak - top)
        old_total = old_sum[head_size : head_size + 1, :]
        new_total = new_sum[2 * head_size : 2 * head_size + 1, late]
        second = (
            old_sum[:head_size, half:] * old_factor
            + new_sum[side * head_size : (side + 1) * head_size, late] * new_factor
        )
        context = jnp.concatenate([old_sum[:head_size, :half], second], axis=1).astype(BF16)
        for part in range(head_size // SLAB):
            slab = head * (head_size // SLAB) + part
            chunk_slabs = (msg_ref.shape[1] - 16) // SLAB
            place = pl.multiple_of((slab % chunk_slabs) * SLAB, SLAB)
            msg_ref[slab // chunk_slabs, pl.ds(place, SLAB), :] = context[
                part * SLAB : (part + 1) * SLAB, :
            ]
        stat_ref[head, 0:1, :] = jnp.concatenate([old_peak[:, :half], top], axis=1)
        stat_ref[head, 1:2, :] = jnp.concatenate(
            [old_total[:, :half], old_total[:, half:] * old_factor + new_total * new_factor], axis=1
        )

    @pl.when(pair == pl.num_programs(0) - 1)
    def _():
        heads = stat_ref.shape[0]
        chunk_rows = msg_ref.shape[1] - 16
        for chunk in range(chunks):
            first = chunk * chunk_rows // head_size
            rows = []
            for head in range(first, first + 3):
                rows += stat_rows(stat_ref[head, 0:1, :], stat_ref[head, 1:2, :])
            rows.append(jnp.zeros_like(rows[0]))
            msg_ref[chunk, chunk_rows:, :] = jnp.concatenate(rows, axis=0).astype(BF16)


def attend(lengths, slope, gathered, keys, values_t, dist, frame_count, columns, beside):
    near, _, tokens = gathered.shape
    rows, width = keys.shape
    head_count = slope.shape[0]
    pair_rows = 2 * (width // head_count)
    keys, values_t = (pltpu.with_memory_space_constraint(x, pltpu.HBM) for x in (keys, values_t))
    return pl.pallas_call(
        functools.partial(
            attend_kernel, frame_count=frame_count, chunks=near, columns=columns, beside=beside
        ),
        grid=(head_count // 2,),
        in_specs=[
            pl.BlockSpec(memory_space=pltpu.SMEM),
            pl.BlockSpec(memory_space=pltpu.SMEM),
            pl.BlockSpec(gathered.shape, lambda p: (0, 0, 0)),
            pl.BlockSpec((rows, pair_rows), lambda p: (0, p)),
            pl.BlockSpec((pair_rows, rows), lambda p: (p, 0)),
            pl.BlockSpec(dist.shape, lambda p: (0, 0)),
        ],
        out_specs=pl.BlockSpec((near, width // near + 16, tokens), lambda p: (0, 0, 0)),
        out_shape=jax.ShapeDtypeStruct((near, width // near + 16, tokens), BF16),
        scratch_shapes=[pltpu.VMEM((head_count, 8, tokens), F32)],
        compiler_params=pltpu.CompilerParams(vmem_limit_bytes=40 << 20),
        name="attend",
    )(lengths, slope, gathered, keys, values_t, dist)


def merge_kernel(odd_ref, in_ref, out_ref):
    sources, rows, tokens = in_ref.shape
    chunk_rows = rows - 16
    stats = [in_ref[:, chunk_rows + r, :].astype(F32) for r in range(3 * STAT_ROWS)]
    tops, totals, factors = [], [], []
    for slot in range(3):
        at = slot * STAT_ROWS
        peak = (stats[at] + stats[at + 1]) + stats[at + 2]
        top = jnp.max(peak, axis=0, keepdims=True)
        factor = jnp.exp(peak - top)
        tops.append(top)
        factors.append(factor)
        totals.append(jnp.sum(factor * (stats[at + 3] + stats[at + 4]), axis=0, keepdims=True))
    odd = odd_ref[0] == 1
    slabs, slab_stats = [], []
    for slab in range(chunk_rows // SLAB):
        even_slot, odd_slot = slab // 2, (slab + 1) // 2
        pick = lambda x: x[even_slot] if even_slot == odd_slot else jnp.where(odd, x[odd_slot], x[even_slot])
        factor = pick(factors)
        total = None
        for source in range(sources):
            part = in_ref[source, slab * SLAB : (slab + 1) * SLAB, :].astype(F32)
            part = part * factor[source : source + 1, :]
            total = part if total is None else total + part
        slabs.append(total)
        slab_stats.append(stat_rows(pick(tops), pick(totals)))
    merged = jnp.concatenate(slabs, axis=0)
    targets, out_rows, lanes = out_ref.shape
    pieces = targets // 2
    piece = chunk_rows // pieces
    for target in range(targets):
        side, at = target // pieces, (target % pieces) * piece
        cut = slice(side * lanes, (side + 1) * lanes)
        rows = slab_stats[at // SLAB] + slab_stats[(at + piece - 1) // SLAB]
        rows = [r[:, cut] for r in rows]
        rows.append(jnp.zeros((out_rows - piece - len(rows), lanes), F32))
        out_ref[target] = jnp.concatenate([merged[at : at + piece, cut]] + rows, axis=0).astype(BF16)


def finish_kernel(bound_ref, in_ref, out_ref, *, piece):
    sources, rows, lanes = in_ref.shape
    stats = [in_ref[:, piece + r, :].astype(F32) for r in range(2 * STAT_ROWS)]
    factors, totals = [], []
    for at in (0, STAT_ROWS):
        peak = (stats[at] + stats[at + 1]) + stats[at + 2]
        factor = jnp.exp(peak - jnp.max(peak, axis=0, keepdims=True))
        factors.append(factor)
        totals.append(jnp.sum(factor * (stats[at + 3] + stats[at + 4]), axis=0, keepdims=True))
    out_rows = out_ref.shape[0]
    row = lax.broadcasted_iota(jnp.int32, (out_rows, lanes), 0)
    first = row < bound_ref[0]
    total = None
    for source in range(sources):
        factor = jnp.where(first, factors[0][source : source + 1, :], factors[1][source : source + 1, :])
        part = in_ref[source, :out_rows, :].astype(F32) * factor
        total = part if total is None else total + part
    context = total / jnp.where(first, totals[0], totals[1])
    out_ref[...] = jnp.where(row < piece, context, 0.0).astype(BF16)


def project_kernel(ctx_ref, w_ref, out_ref):
    pieces, sides = ctx_ref.shape[:2]
    for side in range(sides):
        total = None
        for at in range(pieces):
            part = lax.dot_general(
                ctx_ref[at, side], w_ref[at], (((0,), (0,)), ((), ())), preferred_element_type=F32
            )
            total = part if total is None else total + part
        out_ref[side] = total.astype(BF16)


def whole(kernel, out_shape, scalars, arrays, name):
    return pl.pallas_call(
        kernel,
        in_specs=[pl.BlockSpec(memory_space=pltpu.SMEM)] * len(scalars)
        + [pl.BlockSpec(memory_space=pltpu.VMEM)] * len(arrays),
        out_specs=pl.BlockSpec(memory_space=pltpu.VMEM),
        out_shape=out_shape,
        compiler_params=pltpu.CompilerParams(vmem_limit_bytes=32 << 20),
        name=name,
    )(*scalars, *arrays)


def spread(x, axis):
    copies = jnp.broadcast_to(x[None], (lax.axis_size(axis), *x.shape))
    copies = lax.optimization_barrier(copies)
    return lax.all_to_all(copies, axis, 0, 0)


def local(frames, dec_states, w_query, w_keyval, w_output, head_slope, lengths, positions):
    devices = lax.axis_size(SEQ)
    own_index = lax.axis_index(SEQ)
    across, beside, cores = (lax.axis_size(axis) for axis in SEQ)
    step_count, frame_count, width = frames.shape
    query_rows = dec_states.shape[1]
    tokens = step_count * query_rows
    columns = w_query.shape[1]
    near = beside * cores

    own_queries = lax.dot_general(
        w_query,
        dec_states.reshape(tokens, width),
        (((0,), (1,)), ((), ())),
        preferred_element_type=F32,
    ).astype(BF16)
    padded = jnp.pad(own_queries, ((0, 16 - columns), (0, 0)))
    queries = spread(padded, "seq_0")[:, :columns]
    queries = spread(queries.reshape(across * columns, tokens), "seq_1")
    queries = lax.all_gather(queries, "seq_2").reshape(near, across * columns, tokens)

    frame_rows = frames.reshape(step_count * frame_count, width)
    keys = jnp.dot(frame_rows, w_keyval[:, :width], preferred_element_type=F32).astype(BF16)
    values_t = lax.dot_general(
        w_keyval[:, width:], frame_rows, (((0,), (1,)), ((), ())), preferred_element_type=F32
    ).astype(BF16)

    slot_place = ((own_index + 1) % devices).astype(F32)
    apart = jnp.abs(positions.astype(F32) - slot_place) / devices
    age = jnp.arange(step_count, dtype=F32)[:, None]
    dist = jnp.stack([(apart + age).reshape(tokens), apart.reshape(tokens)])
    dist = jnp.pad(dist, ((0, 6), (0, 0)))
    own_lengths = lax.dynamic_slice(lengths, (0, own_index), (step_count, 1)).reshape(step_count)

    odd = (lax.axis_index(("seq_1", "seq_2")) % 2).astype(jnp.int32).reshape(1)
    piece = 2 * width // devices
    at = (lax.axis_index("seq_0") % (across // 2)) * piece
    bound = (SLAB - at % SLAB).astype(jnp.int32).reshape(1)
    weights = w_output.reshape(beside, cores, across // 2, piece, columns)
    weights = jnp.pad(weights, ((0, 0), (0, 0), (0, 0), (0, 24 - piece), (0, 0)))
    weights = weights.transpose(1, 0, 2, 3, 4).reshape(near, across // 2 * 24, columns)
    queries, weights, odd, bound, dist, own_lengths = lax.optimization_barrier(
        (queries, weights, odd, bound, dist, own_lengths)
    )
    message = attend(
        own_lengths, head_slope, queries, keys, values_t, dist, frame_count, columns, beside
    )
    message = lax.all_to_all(message, ("seq_1", "seq_2"), 0, 0)
    message = whole(
        merge_kernel,
        jax.ShapeDtypeStruct((across, SLAB, tokens // 2), BF16),
        [odd],
        [message],
        "merge",
    )
    message = lax.all_to_all(message, "seq_0", 0, 0)
    context = whole(
        functools.partial(finish_kernel, piece=piece),
        jax.ShapeDtypeStruct((24, tokens // 2), BF16),
        [bound],
        [message],
        "finish",
    )
    context = spread(context, "seq_0")
    context = spread(context.reshape(across * 24, tokens // 2), "seq_1")
    context = lax.all_gather(context, "seq_2")
    context = context.reshape(near, 2, across // 2 * 24, tokens // 2)
    return whole(
        project_kernel,
        jax.ShapeDtypeStruct((step_count, query_rows, columns), BF16),
        [],
        [context, weights],
        "project",
    )


def solution(mesh):
    finer = Mesh(
        mesh.devices.reshape(mesh.shape["grp"], 16, 4, 2), ("grp", "seq_0", "seq_1", "seq_2")
    )
    return jax.shard_map(
        local,
        mesh=finer,
        in_specs=(
            P("grp", SEQ, None),
            P(None, "grp", None),
            P(None, SEQ),
            P(),
            P(None, SEQ),
            P(),
            P("grp", None),
            P(None, "grp"),
        ),
        out_specs=P(None, "grp", SEQ),
        check_vma=False,
    )
```

```python
import functools
import math

import jax
import jax.numpy as jnp
from jax import lax
from jax.experimental import pallas as pl
from jax.experimental.pallas import tpu as pltpu
from jax.sharding import Mesh
from jax.sharding import PartitionSpec as P

SEQ = ("seq_0", "seq_1", "seq_2")
BF16 = jnp.bfloat16
F32 = jnp.float32
SLAB = 32
PEAK_ROWS = 3
STAT_ROWS = 5
PAIRS = 2
AHEAD = 3
LOG2E = math.log2(math.e)


def split_rows(x, count):
    rows = []
    for _ in range(count):
        part = x.astype(BF16).astype(F32)
        rows.append(part)
        x = x - part
    return rows


def stat_rows(peak, total):
    return split_rows(peak, PEAK_ROWS) + split_rows(total, STAT_ROWS - PEAK_ROWS)


def floor_div(x, n):
    return (x * (2**19 // n + 1)) >> 19


def pair_queries(pair, gathered_ref, rows, columns):
    near, held, _ = gathered_ref.shape
    window = 48
    span = near * columns
    first = jnp.minimum((pair * rows // span) * columns // 16, (held - window) // 16)
    start = pl.multiple_of(first * 16, 16)
    pieces = [gathered_ref[at, pl.ds(start, window), :] for at in range(near)]
    shape = (rows, near * window)
    at = pair * rows + lax.broadcasted_iota(jnp.int32, (rows, 128), 0)
    far = floor_div(at, span)
    rest = at - far * span
    owner = floor_div(rest, columns)
    column = rest - owner * columns
    source = owner * window + far * columns + column - first * 16
    source = jnp.concatenate([source] * (near * window // 128), axis=1)
    picked = (lax.broadcasted_iota(jnp.int32, shape, 1) == source).astype(F32).astype(BF16)
    queries = jnp.dot(picked, jnp.concatenate(pieces, axis=0), preferred_element_type=F32)
    return queries.astype(BF16)


def attend_kernel(
    lengths_ref,
    slope_ref,
    gathered_ref,
    k_ref,
    vt_ref,
    dist_ref,
    msg_ref,
    stat_ref,
    query_ref,
    *,
    frame_count,
    chunks,
    columns,
    head_size,
):
    step, last = pl.program_id(0), pl.num_programs(0) - 1
    lanes = 2 * head_size
    pairs = k_ref.shape[1] // lanes
    tokens = gathered_ref.shape[2]
    half = tokens // 2
    scale = 1.0 / math.sqrt(head_size)

    def find_queries(step_at, slot):
        for pair in range(pairs):
            query_ref[slot, pair] = pair_queries(
                step_at * pairs + pair, gathered_ref, lanes, columns
            )

    @pl.when(step == 0)
    def _():
        find_queries(0, 0)

    row = lax.broadcasted_iota(jnp.int32, (frame_count, lanes), 0)
    lane = lax.broadcasted_iota(jnp.int32, (frame_count, lanes), 1)
    invalid = [
        jnp.where(jnp.logical_and(row >= lengths_ref[block], lane == 0), 1.0, 0.0).astype(BF16)
        for block in range(2)
    ]
    floor_row = lax.broadcasted_iota(jnp.int32, (lanes, tokens), 0)
    floor = jnp.where(floor_row == 0, -1e30, 0.0).astype(BF16)
    ones = jnp.ones((16, frame_count), BF16)
    zeros = jnp.zeros((head_size, tokens), BF16)
    zeros_half = jnp.zeros((head_size, half), BF16)

    units = [(pair, part) for pair in range(pairs) for part in range(3)]

    def score(pair, part):
        block = 1 if part == 0 else 0
        keys = k_ref[block * frame_count : (block + 1) * frame_count, pair * lanes : (pair + 1) * lanes]
        first = query_ref[step % 2, pair, :head_size, :]
        second = query_ref[step % 2, pair, head_size:, :]
        if part == 0:
            rows = [
                jnp.concatenate([first[:, half:], zeros_half], axis=1),
                jnp.concatenate([zeros_half, second[:, half:]], axis=1),
            ]
        else:
            rows = [first, zeros] if part == 1 else [zeros, second]
        return jnp.dot(
            jnp.concatenate([keys, invalid[block]], axis=1),
            jnp.concatenate(rows + [floor], axis=0),
            preferred_element_type=F32,
        )

    def weigh(pair, part, scores):
        peak = jnp.max(scores, axis=0, keepdims=True)
        weights = jnp.exp2((scores - peak) * (scale * LOG2E)).astype(BF16)
        top = pair * lanes
        if part == 0:
            values = vt_ref[top : top + lanes, frame_count:]
        else:
            start = top + (part - 1) * head_size
            values = vt_ref[start : start + head_size, :frame_count]
        values = jnp.concatenate([values, ones], axis=0)
        return peak * scale, jnp.dot(values, weights, preferred_element_type=F32)

    def emit(pair, side, new, old):
        head = (step * pairs + pair) * 2 + side
        (new_peak, new_sum), (old_peak, old_sum) = new, old
        slope = slope_ref[head]
        late = slice(side * half, (side + 1) * half)
        old_peak = old_peak - slope * dist_ref[0:1, :]
        late_peak = new_peak[:, late] - slope * dist_ref[1:2, half:]
        top = jnp.maximum(old_peak[:, half:], late_peak)
        old_factor = jnp.exp(old_peak[:, half:] - top)
        new_factor = jnp.exp(late_peak - top)
        old_total = old_sum[head_size : head_size + 1, :]
        new_total = new_sum[lanes : lanes + 1, late]
        second = (
            old_sum[:head_size, half:] * old_factor
            + new_sum[side * head_size : (side + 1) * head_size, late] * new_factor
        )
        context = jnp.concatenate([old_sum[:head_size, :half], second], axis=1).astype(BF16)
        for part in range(head_size // SLAB):
            slab = head * (head_size // SLAB) + part
            chunk_slabs = (msg_ref.shape[1] - 16) // SLAB
            place = pl.multiple_of((slab % chunk_slabs) * SLAB, SLAB)
            msg_ref[slab // chunk_slabs, pl.ds(place, SLAB), :] = context[
                part * SLAB : (part + 1) * SLAB, :
            ]
        stat_ref[head, 0:1, :] = jnp.concatenate([old_peak[:, :half], top], axis=1)
        stat_ref[head, 1:2, :] = jnp.concatenate(
            [old_total[:, :half], old_total[:, half:] * old_factor + new_total * new_factor], axis=1
        )

    ahead = [score(*units[at]) for at in range(AHEAD)]
    done = {}
    for at, (pair, part) in enumerate(units):
        if at + AHEAD < len(units):
            ahead.append(score(*units[at + AHEAD]))
        if at == 1:
            find_queries(jnp.minimum(step + 1, last), 1 - step % 2)
        done[part] = weigh(pair, part, ahead[at])
        ahead[at] = None
        if part > 0:
            emit(pair, part - 1, done[0], done[part])

    @pl.when(step == last)
    def _():
        chunk_rows = msg_ref.shape[1] - 16
        for chunk in range(chunks):
            first = chunk * chunk_rows // head_size
            rows = []
            for head in range(first, first + 3):
                rows += stat_rows(stat_ref[head, 0:1, :], stat_ref[head, 1:2, :])
            rows.append(jnp.zeros_like(rows[0]))
            msg_ref[chunk, chunk_rows:, :] = jnp.concatenate(rows, axis=0).astype(BF16)


def attend(lengths, slope, gathered, keys, values_t, dist, frame_count, columns):
    near, _, tokens = gathered.shape
    rows, width = keys.shape
    head_count = slope.shape[0]
    head_size = width // head_count
    step_rows = PAIRS * 2 * head_size
    keys, values_t = (pltpu.with_memory_space_constraint(x, pltpu.HBM) for x in (keys, values_t))
    return pl.pallas_call(
        functools.partial(
            attend_kernel,
            frame_count=frame_count,
            chunks=near,
            columns=columns,
            head_size=head_size,
        ),
        grid=(width // step_rows,),
        in_specs=[
            pl.BlockSpec(memory_space=pltpu.SMEM),
            pl.BlockSpec(memory_space=pltpu.SMEM),
            pl.BlockSpec(gathered.shape, lambda p: (0, 0, 0)),
            pl.BlockSpec((rows, step_rows), lambda p: (0, p)),
            pl.BlockSpec((step_rows, rows), lambda p: (p, 0)),
            pl.BlockSpec(dist.shape, lambda p: (0, 0)),
        ],
        out_specs=pl.BlockSpec((near, width // near + 16, tokens), lambda p: (0, 0, 0)),
        out_shape=jax.ShapeDtypeStruct((near, width // near + 16, tokens), BF16),
        scratch_shapes=[
            pltpu.VMEM((head_count, 8, tokens), F32),
            pltpu.VMEM((2, PAIRS, 2 * head_size, tokens), BF16),
        ],
        compiler_params=pltpu.CompilerParams(vmem_limit_bytes=40 << 20),
        name="attend",
    )(lengths, slope, gathered, keys, values_t, dist)


def merge_kernel(odd_ref, in_ref, out_ref):
    sources, rows, tokens = in_ref.shape
    chunk_rows = rows - 16
    stats = [in_ref[:, chunk_rows + r, :].astype(F32) for r in range(3 * STAT_ROWS)]
    tops, totals, factors = [], [], []
    for slot in range(3):
        at = slot * STAT_ROWS
        peak = (stats[at] + stats[at + 1]) + stats[at + 2]
        top = jnp.max(peak, axis=0, keepdims=True)
        factor = jnp.exp(peak - top)
        tops.append(top)
        factors.append(factor)
        totals.append(jnp.sum(factor * (stats[at + 3] + stats[at + 4]), axis=0, keepdims=True))
    odd = odd_ref[0] == 1
    slabs, slab_stats = [], []
    for slab in range(chunk_rows // SLAB):
        even_slot, odd_slot = slab // 2, (slab + 1) // 2
        pick = lambda x: x[even_slot] if even_slot == odd_slot else jnp.where(odd, x[odd_slot], x[even_slot])
        factor = pick(factors)
        total = None
        for source in range(sources):
            part = in_ref[source, slab * SLAB : (slab + 1) * SLAB, :].astype(F32)
            part = part * factor[source : source + 1, :]
            total = part if total is None else total + part
        slabs.append(total)
        slab_stats.append(stat_rows(pick(tops), pick(totals)))
    merged = jnp.concatenate(slabs, axis=0)
    targets, out_rows, lanes = out_ref.shape
    pieces = targets // 2
    piece = chunk_rows // pieces
    for target in range(targets):
        side, at = target // pieces, (target % pieces) * piece
        cut = slice(side * lanes, (side + 1) * lanes)
        rows = slab_stats[at // SLAB] + slab_stats[(at + piece - 1) // SLAB]
        rows = [r[:, cut] for r in rows]
        rows.append(jnp.zeros((out_rows - piece - len(rows), lanes), F32))
        out_ref[target] = jnp.concatenate([merged[at : at + piece, cut]] + rows, axis=0).astype(BF16)


def finish_kernel(bound_ref, in_ref, out_ref, *, piece):
    sources, rows, lanes = in_ref.shape
    stats = [in_ref[:, piece + r, :].astype(F32) for r in range(2 * STAT_ROWS)]
    factors, totals = [], []
    for at in (0, STAT_ROWS):
        peak = (stats[at] + stats[at + 1]) + stats[at + 2]
        factor = jnp.exp(peak - jnp.max(peak, axis=0, keepdims=True))
        factors.append(factor)
        totals.append(jnp.sum(factor * (stats[at + 3] + stats[at + 4]), axis=0, keepdims=True))
    out_rows = out_ref.shape[0]
    row = lax.broadcasted_iota(jnp.int32, (out_rows, lanes), 0)
    first = row < bound_ref[0]
    total = None
    for source in range(sources):
        factor = jnp.where(first, factors[0][source : source + 1, :], factors[1][source : source + 1, :])
        part = in_ref[source, :out_rows, :].astype(F32) * factor
        total = part if total is None else total + part
    context = total / jnp.where(first, totals[0], totals[1])
    out_ref[...] = jnp.where(row < piece, context, 0.0).astype(BF16)


def project_kernel(ctx_ref, w_ref, out_ref):
    pieces, sides = ctx_ref.shape[:2]
    for side in range(sides):
        total = None
        for at in range(pieces):
            part = lax.dot_general(
                ctx_ref[at, side], w_ref[at], (((0,), (0,)), ((), ())), preferred_element_type=F32
            )
            total = part if total is None else total + part
        out_ref[side] = total.astype(BF16)


def whole(kernel, out_shape, scalars, arrays, name):
    return pl.pallas_call(
        kernel,
        in_specs=[pl.BlockSpec(memory_space=pltpu.SMEM)] * len(scalars)
        + [pl.BlockSpec(memory_space=pltpu.VMEM)] * len(arrays),
        out_specs=pl.BlockSpec(memory_space=pltpu.VMEM),
        out_shape=out_shape,
        compiler_params=pltpu.CompilerParams(vmem_limit_bytes=32 << 20),
        name=name,
    )(*scalars, *arrays)


def spread(x, axis):
    copies = jnp.broadcast_to(x[None], (lax.axis_size(axis), *x.shape))
    copies = lax.optimization_barrier(copies)
    return lax.all_to_all(copies, axis, 0, 0)


def local(frames, dec_states, w_query, w_keyval, w_output, head_slope, lengths, positions):
    devices = lax.axis_size(SEQ)
    own_index = lax.axis_index(SEQ)
    across, beside, cores = (lax.axis_size(axis) for axis in SEQ)
    step_count, frame_count, width = frames.shape
    query_rows = dec_states.shape[1]
    tokens = step_count * query_rows
    columns = w_query.shape[1]
    near = beside * cores

    own_queries = lax.dot_general(
        w_query,
        dec_states.reshape(tokens, width),
        (((0,), (1,)), ((), ())),
        preferred_element_type=F32,
    ).astype(BF16)
    padded = jnp.pad(own_queries, ((0, 16 - columns), (0, 0)))
    queries = spread(padded, "seq_0")[:, :columns]
    queries, late_frames = lax.optimization_barrier((queries, frames))
    queries = spread(queries.reshape(across * columns, tokens), SEQ[1:])

    frame_rows = frames.reshape(step_count * frame_count, width)
    keys = jnp.dot(frame_rows, w_keyval[:, :width], preferred_element_type=F32).astype(BF16)
    late_rows = late_frames.reshape(step_count * frame_count, width)
    values_t = lax.dot_general(
        w_keyval[:, width:], late_rows, (((0,), (1,)), ((), ())), preferred_element_type=F32
    ).astype(BF16)

    slot_place = ((own_index + 1) % devices).astype(F32)
    apart = jnp.abs(positions.astype(F32) - slot_place) / devices
    age = jnp.arange(step_count, dtype=F32)[:, None]
    dist = jnp.stack([(apart + age).reshape(tokens), apart.reshape(tokens)])
    dist = jnp.pad(dist, ((0, 6), (0, 0)))
    own_lengths = lax.dynamic_slice(lengths, (0, own_index), (step_count, 1)).reshape(step_count)

    odd = (lax.axis_index(("seq_1", "seq_2")) % 2).astype(jnp.int32).reshape(1)
    piece = 2 * width // devices
    at = (lax.axis_index("seq_0") % (across // 2)) * piece
    bound = (SLAB - at % SLAB).astype(jnp.int32).reshape(1)
    weights = w_output.reshape(beside, cores, across // 2, piece, columns)
    weights = jnp.pad(weights, ((0, 0), (0, 0), (0, 0), (0, 24 - piece), (0, 0)))
    weights = weights.transpose(1, 0, 2, 3, 4).reshape(near, across // 2 * 24, columns)
    queries, weights, odd, bound, dist, own_lengths = lax.optimization_barrier(
        (queries, weights, odd, bound, dist, own_lengths)
    )
    message = attend(
        own_lengths, head_slope, queries, keys, values_t, dist, frame_count, columns
    )
    message = lax.all_to_all(message, ("seq_1", "seq_2"), 0, 0)
    message = whole(
        merge_kernel,
        jax.ShapeDtypeStruct((across, SLAB, tokens // 2), BF16),
        [odd],
        [message],
        "merge",
    )
    message = lax.all_to_all(message, "seq_0", 0, 0)
    context = whole(
        functools.partial(finish_kernel, piece=piece),
        jax.ShapeDtypeStruct((24, tokens // 2), BF16),
        [bound],
        [message],
        "finish",
    )
    context = spread(context, "seq_0")
    context = spread(context.reshape(across * 24, tokens // 2), "seq_1")
    context = lax.all_gather(context, "seq_2")
    context = context.reshape(near, 2, across // 2 * 24, tokens // 2)
    return whole(
        project_kernel,
        jax.ShapeDtypeStruct((step_count, query_rows, columns), BF16),
        [],
        [context, weights],
        "project",
    )


def solution(mesh):
    finer = Mesh(
        mesh.devices.reshape(mesh.shape["grp"], 16, 4, 2), ("grp", "seq_0", "seq_1", "seq_2")
    )
    return jax.shard_map(
        local,
        mesh=finer,
        in_specs=(
            P("grp", SEQ, None),
            P(None, "grp", None),
            P(None, SEQ),
            P(),
            P(None, SEQ),
            P(),
            P("grp", None),
            P(None, "grp"),
        ),
        out_specs=P(None, "grp", SEQ),
        check_vma=False,
    )
```

```python
import functools
import math

import jax
import jax.numpy as jnp
from jax import lax
from jax.experimental import pallas as pl
from jax.experimental.pallas import tpu as pltpu
from jax.sharding import Mesh
from jax.sharding import PartitionSpec as P

SEQ = ("seq_0", "seq_1", "seq_2")
BF16 = jnp.bfloat16
F32 = jnp.float32
SLAB = 32
PEAK_ROWS = 3
STAT_ROWS = 5
PAIRS = 2
AHEAD = 3
LOG2E = math.log2(math.e)


def split_rows(x, count):
    rows = []
    for _ in range(count):
        part = x.astype(BF16).astype(F32)
        rows.append(part)
        x = x - part
    return rows


def stat_rows(peak, total):
    return split_rows(peak, PEAK_ROWS) + split_rows(total, STAT_ROWS - PEAK_ROWS)


def floor_div(x, n):
    return (x * (2**19 // n + 1)) >> 19


def pair_queries(pair, gathered_ref, rows, columns):
    near, held, _ = gathered_ref.shape
    window = 48
    span = near * columns
    first = jnp.minimum((pair * rows // span) * columns // 16, (held - window) // 16)
    start = pl.multiple_of(first * 16, 16)
    pieces = [gathered_ref[at, pl.ds(start, window), :] for at in range(near)]
    shape = (rows, near * window)
    at = pair * rows + lax.broadcasted_iota(jnp.int32, (rows, 128), 0)
    far = floor_div(at, span)
    rest = at - far * span
    owner = floor_div(rest, columns)
    column = rest - owner * columns
    source = owner * window + far * columns + column - first * 16
    source = jnp.concatenate([source] * (near * window // 128), axis=1)
    picked = (lax.broadcasted_iota(jnp.int32, shape, 1) == source).astype(F32).astype(BF16)
    queries = jnp.dot(picked, jnp.concatenate(pieces, axis=0), preferred_element_type=F32)
    return queries.astype(BF16)


def attend_kernel(
    lengths_ref,
    slope_ref,
    core_ref,
    gathered_ref,
    k_ref,
    vt_ref,
    dist_ref,
    mine_ref,
    theirs_ref,
    msg_ref,
    stat_ref,
    query_ref,
    *,
    frame_count,
    chunks,
    columns,
    head_size,
):
    step, last = pl.program_id(0), pl.num_programs(0) - 1
    lanes = 2 * head_size
    pairs = k_ref.shape[1] // lanes
    tokens = gathered_ref.shape[2]
    half = tokens // 2
    scale = 1.0 / math.sqrt(head_size)

    def find_queries(step_at, slot):
        for pair in range(pairs):
            query_ref[slot, pair] = pair_queries(
                step_at * pairs + pair, gathered_ref, lanes, columns
            )

    @pl.when(step == 0)
    def _():
        find_queries(0, 0)

    row = lax.broadcasted_iota(jnp.int32, (frame_count, lanes), 0)
    lane = lax.broadcasted_iota(jnp.int32, (frame_count, lanes), 1)
    invalid = [
        jnp.where(jnp.logical_and(row >= lengths_ref[block], lane == 0), 1.0, 0.0).astype(BF16)
        for block in range(2)
    ]
    floor_row = lax.broadcasted_iota(jnp.int32, (lanes, tokens), 0)
    floor = jnp.where(floor_row == 0, -1e30, 0.0).astype(BF16)
    ones = jnp.ones((16, frame_count), BF16)
    zeros = jnp.zeros((head_size, tokens), BF16)
    zeros_half = jnp.zeros((head_size, half), BF16)

    units = [(pair, part) for pair in range(pairs) for part in range(3)]

    def score(pair, part):
        block = 1 if part == 0 else 0
        keys = k_ref[block * frame_count : (block + 1) * frame_count, pair * lanes : (pair + 1) * lanes]
        first = query_ref[step % 2, pair, :head_size, :]
        second = query_ref[step % 2, pair, head_size:, :]
        if part == 0:
            rows = [
                jnp.concatenate([first[:, half:], zeros_half], axis=1),
                jnp.concatenate([zeros_half, second[:, half:]], axis=1),
            ]
        else:
            rows = [first, zeros] if part == 1 else [zeros, second]
        return jnp.dot(
            jnp.concatenate([keys, invalid[block]], axis=1),
            jnp.concatenate(rows + [floor], axis=0),
            preferred_element_type=F32,
        )

    def weigh(pair, part, scores):
        peak = jnp.max(scores, axis=0, keepdims=True)
        weights = jnp.exp2((scores - peak) * (scale * LOG2E)).astype(BF16)
        top = pair * lanes
        if part == 0:
            values = vt_ref[top : top + lanes, frame_count:]
        else:
            start = top + (part - 1) * head_size
            values = vt_ref[start : start + head_size, :frame_count]
        values = jnp.concatenate([values, ones], axis=0)
        return peak * scale, jnp.dot(values, weights, preferred_element_type=F32)

    def emit(pair, side, new, old):
        head = (step * pairs + pair) * 2 + side
        (new_peak, new_sum), (old_peak, old_sum) = new, old
        slope = slope_ref[head]
        late = slice(side * half, (side + 1) * half)
        old_peak = old_peak - slope * dist_ref[0:1, :]
        late_peak = new_peak[:, late] - slope * dist_ref[1:2, half:]
        top = jnp.maximum(old_peak[:, half:], late_peak)
        old_factor = jnp.exp(old_peak[:, half:] - top)
        new_factor = jnp.exp(late_peak - top)
        old_total = old_sum[head_size : head_size + 1, :]
        new_total = new_sum[lanes : lanes + 1, late]
        second = (
            old_sum[:head_size, half:] * old_factor
            + new_sum[side * head_size : (side + 1) * head_size, late] * new_factor
        )
        context = jnp.concatenate([old_sum[:head_size, :half], second], axis=1)
        for part in range(head_size // SLAB):
            slab = head * (head_size // SLAB) + part
            chunk_slabs = (msg_ref.shape[2] - 8) // SLAB
            chunk = slab // chunk_slabs
            place = pl.multiple_of((slab % chunk_slabs) * SLAB, SLAB)
            msg_ref[(chunk + core_ref[0]) % 2, chunk // 2, pl.ds(place, SLAB), :] = context[
                part * SLAB : (part + 1) * SLAB, :
            ]
        stat_ref[head, 0:1, :] = jnp.concatenate([old_peak[:, :half], top], axis=1)
        stat_ref[head, 1:2, :] = jnp.concatenate(
            [old_total[:, :half], old_total[:, half:] * old_factor + new_total * new_factor], axis=1
        )

    ahead = [score(*units[at]) for at in range(AHEAD)]
    done = {}
    for at, (pair, part) in enumerate(units):
        if at + AHEAD < len(units):
            ahead.append(score(*units[at + AHEAD]))
        if at == 1:
            find_queries(jnp.minimum(step + 1, last), 1 - step % 2)
        done[part] = weigh(pair, part, ahead[at])
        ahead[at] = None
        if part > 0:
            emit(pair, part - 1, done[0], done[part])

    @pl.when(step == last)
    def _():
        chunk_rows = msg_ref.shape[2] - 8
        for chunk in range(chunks):
            first = chunk * chunk_rows // head_size
            rows = [stat_ref[head, 0:2, :] for head in range(first, first + 3)]
            rows.append(jnp.zeros_like(rows[0]))
            msg_ref[(chunk + core_ref[0]) % 2, chunk // 2, chunk_rows:, :] = jnp.concatenate(
                rows, axis=0
            )
        mine_ref[...] = msg_ref[0]
        theirs_ref[...] = msg_ref[1]


def attend(lengths, slope, core, gathered, keys, values_t, dist, frame_count, columns):
    near, _, tokens = gathered.shape
    rows, width = keys.shape
    head_count = slope.shape[0]
    head_size = width // head_count
    step_rows = PAIRS * 2 * head_size
    part = (near // 2, width // near + 8, tokens)
    keys, values_t = (pltpu.with_memory_space_constraint(x, pltpu.HBM) for x in (keys, values_t))
    return pl.pallas_call(
        functools.partial(
            attend_kernel,
            frame_count=frame_count,
            chunks=near,
            columns=columns,
            head_size=head_size,
        ),
        grid=(width // step_rows,),
        in_specs=[
            pl.BlockSpec(memory_space=pltpu.SMEM),
            pl.BlockSpec(memory_space=pltpu.SMEM),
            pl.BlockSpec(memory_space=pltpu.SMEM),
            pl.BlockSpec(gathered.shape, lambda p: (0, 0, 0)),
            pl.BlockSpec((rows, step_rows), lambda p: (0, p)),
            pl.BlockSpec((step_rows, rows), lambda p: (p, 0)),
            pl.BlockSpec(dist.shape, lambda p: (0, 0)),
        ],
        out_specs=[pl.BlockSpec(part, lambda p: (0, 0, 0))] * 2,
        out_shape=[jax.ShapeDtypeStruct(part, F32)] * 2,
        scratch_shapes=[
            pltpu.VMEM((2, *part), F32),
            pltpu.VMEM((head_count, 8, tokens), F32),
            pltpu.VMEM((2, PAIRS, 2 * head_size, tokens), BF16),
        ],
        compiler_params=pltpu.CompilerParams(vmem_limit_bytes=40 << 20),
        name="attend",
    )(lengths, slope, core, gathered, keys, values_t, dist)


def slab_value(values, slab, odd):
    even_slot, odd_slot = slab // 2, (slab + 1) // 2
    if even_slot == odd_slot:
        return values[even_slot]
    return jnp.where(odd, values[odd_slot], values[even_slot])


def join_kernel(odd_ref, mine_ref, theirs_ref, out_ref):
    chunks, rows, tokens = mine_ref.shape
    chunk_rows = rows - 8
    odd = odd_ref[0] == 1
    for chunk in range(chunks):
        own, other, stats = [], [], []
        for slot in range(3):
            at = chunk_rows + 2 * slot
            peak, total = mine_ref[chunk, at : at + 1, :], mine_ref[chunk, at + 1 : at + 2, :]
            peak_two = theirs_ref[chunk, at : at + 1, :]
            total_two = theirs_ref[chunk, at + 1 : at + 2, :]
            top = jnp.maximum(peak, peak_two)
            own.append(jnp.exp(peak - top))
            other.append(jnp.exp(peak_two - top))
            stats += stat_rows(top, total * own[slot] + total_two * other[slot])
        for slab in range(chunk_rows // SLAB):
            cut = slice(slab * SLAB, (slab + 1) * SLAB)
            joined = mine_ref[chunk, cut, :] * slab_value(own, slab, odd)
            joined = joined + theirs_ref[chunk, cut, :] * slab_value(other, slab, odd)
            out_ref[chunk, cut, :] = joined.astype(BF16)
        stats.append(jnp.zeros_like(stats[0]))
        out_ref[chunk, chunk_rows:, :] = jnp.concatenate(stats, axis=0).astype(BF16)


def merge_kernel(odd_ref, in_ref, out_ref):
    sources, rows, tokens = in_ref.shape
    chunk_rows = rows - 16
    stats = [in_ref[:, chunk_rows + r, :].astype(F32) for r in range(3 * STAT_ROWS)]
    tops, totals, factors = [], [], []
    for slot in range(3):
        at = slot * STAT_ROWS
        peak = (stats[at] + stats[at + 1]) + stats[at + 2]
        top = jnp.max(peak, axis=0, keepdims=True)
        factor = jnp.exp(peak - top)
        total = jnp.sum(factor * (stats[at + 3] + stats[at + 4]), axis=0, keepdims=True)
        rounded = total.astype(BF16).astype(F32)
        tops.append(top)
        totals.append(rounded)
        factors.append(factor * (rounded / total))
    odd = odd_ref[0] == 1
    slabs, slab_stats = [], []
    for slab in range(chunk_rows // SLAB):
        factor = slab_value(factors, slab, odd)
        merged = None
        for source in range(sources):
            part = in_ref[source, slab * SLAB : (slab + 1) * SLAB, :].astype(F32)
            part = part * factor[source : source + 1, :]
            merged = part if merged is None else merged + part
        slabs.append(merged)
        rows = split_rows(slab_value(tops, slab, odd), PEAK_ROWS)
        slab_stats.append(jnp.concatenate(rows + [slab_value(totals, slab, odd)], axis=0))
    merged = jnp.concatenate(slabs, axis=0)
    targets, tile, width = out_ref.shape
    lanes = tokens // 2
    pieces = targets // 2
    piece = chunk_rows // pieces
    for target in range(targets):
        side, at = target // pieces, (target % pieces) * piece
        cut = slice(side * lanes, (side + 1) * lanes)
        tiles = [merged[at + r : at + r + tile, cut] for r in range(0, piece, tile)]
        tiles += [slab_stats[at // SLAB][:, cut], slab_stats[(at + piece - 1) // SLAB][:, cut]]
        out_ref[target] = jnp.concatenate(tiles, axis=1).astype(BF16)


def finish_kernel(bound_ref, in_ref, out_ref):
    tile, width = out_ref.shape
    lanes = (in_ref.shape[2] - width) // 2
    factors, totals = [], []
    for head in range(2):
        cut = slice(width + head * lanes, width + (head + 1) * lanes)
        stats = in_ref[:, :, cut].astype(F32)
        peak = (stats[:, 0:1, :] + stats[:, 1:2, :]) + stats[:, 2:3, :]
        factor = jnp.exp(peak - jnp.max(peak, axis=0, keepdims=True))
        factors.append(factor)
        totals.append(jnp.sum(factor * stats[:, 3:4, :], axis=0))
    for at in range(width // lanes):
        cut = slice(at * lanes, (at + 1) * lanes)
        first = at * tile < bound_ref[0]
        factor = jnp.where(first, factors[0], factors[1])
        context = jnp.sum(in_ref[:, :, cut].astype(F32) * factor, axis=0)
        out_ref[:, cut] = (context / jnp.where(first, totals[0], totals[1])).astype(BF16)


def project_kernel(ctx_ref, w_ref, out_ref, rows_ref):
    cores, beside, targets, tile, width = ctx_ref.shape
    sides, _, lanes = rows_ref.shape
    pieces = targets // sides
    piece = width // lanes * tile
    for core in range(cores):
        for column in range(beside):
            chunk = column * cores + core
            for target in range(targets):
                held = ctx_ref[core, column, target].astype(F32)
                top = (chunk * pieces + target % pieces) * piece
                for at in range(width // lanes):
                    start = top + at * tile
                    rows_ref[target // pieces, start : start + tile, :] = held[
                        :, at * lanes : (at + 1) * lanes
                    ]
    for side in range(sides):
        out = jnp.dot(w_ref[...], rows_ref[side].astype(BF16), preferred_element_type=F32)
        out_ref[:, side, :] = out.astype(BF16)


def whole(kernel, out_shape, scalars, arrays, name, scratch=()):
    return pl.pallas_call(
        kernel,
        in_specs=[pl.BlockSpec(memory_space=pltpu.SMEM)] * len(scalars)
        + [pl.BlockSpec(memory_space=pltpu.VMEM)] * len(arrays),
        out_specs=pl.BlockSpec(memory_space=pltpu.VMEM),
        out_shape=out_shape,
        scratch_shapes=scratch,
        compiler_params=pltpu.CompilerParams(vmem_limit_bytes=32 << 20),
        name=name,
    )(*scalars, *arrays)


def spread(x, axis):
    copies = jnp.broadcast_to(x[None], (lax.axis_size(axis), *x.shape))
    copies = lax.optimization_barrier(copies)
    return lax.all_to_all(copies, axis, 0, 0)


def local(frames, dec_states, w_query, w_keyval, w_output, head_slope, lengths, positions):
    devices = lax.axis_size(SEQ)
    own_index = lax.axis_index(SEQ)
    across, beside, cores = (lax.axis_size(axis) for axis in SEQ)
    step_count, frame_count, width = frames.shape
    query_rows = dec_states.shape[1]
    tokens = step_count * query_rows
    columns = w_query.shape[1]
    near = beside * cores

    own_queries = lax.dot_general(
        w_query,
        dec_states.reshape(tokens, width),
        (((0,), (1,)), ((), ())),
        preferred_element_type=F32,
    ).astype(BF16)
    padded = jnp.pad(own_queries, ((0, 16 - columns), (0, 0)))
    queries = spread(padded, "seq_0")[:, :columns]
    queries, late_frames = lax.optimization_barrier((queries, frames))
    queries = spread(queries.reshape(across * columns, tokens), SEQ[1:])

    frame_rows = frames.reshape(step_count * frame_count, width)
    keys = jnp.dot(frame_rows, w_keyval[:, :width], preferred_element_type=F32).astype(BF16)
    late_rows = late_frames.reshape(step_count * frame_count, width)
    values_t = lax.dot_general(
        w_keyval[:, width:], late_rows, (((0,), (1,)), ((), ())), preferred_element_type=F32
    ).astype(BF16)

    slot_place = ((own_index + 1) % devices).astype(F32)
    apart = jnp.abs(positions.astype(F32) - slot_place) / devices
    age = jnp.arange(step_count, dtype=F32)[:, None]
    dist = jnp.stack([(apart + age).reshape(tokens), apart.reshape(tokens)])
    dist = jnp.pad(dist, ((0, 6), (0, 0)))
    own_lengths = lax.dynamic_slice(lengths, (0, own_index), (step_count, 1)).reshape(step_count)

    odd = (lax.axis_index(("seq_1", "seq_2")) % 2).astype(jnp.int32).reshape(1)
    piece = 2 * width // devices
    at = (lax.axis_index("seq_0") % (across // 2)) * piece
    bound = (SLAB - at % SLAB).astype(jnp.int32).reshape(1)
    core = lax.axis_index("seq_2").astype(jnp.int32).reshape(1)
    queries, odd, bound, core, dist, own_lengths = lax.optimization_barrier(
        (queries, odd, bound, core, dist, own_lengths)
    )
    mine, theirs = attend(
        own_lengths, head_slope, core, queries, keys, values_t, dist, frame_count, columns
    )
    theirs = lax.ppermute(theirs, "seq_2", [(at, cores - 1 - at) for at in range(cores)])
    message = whole(
        join_kernel,
        jax.ShapeDtypeStruct((beside, width // near + 16, tokens), BF16),
        [odd],
        [mine, theirs],
        "join",
    )
    message = lax.all_to_all(message, "seq_1", 0, 0)
    lanes = tokens // 2
    tile = 4
    message = whole(
        merge_kernel,
        jax.ShapeDtypeStruct((across, tile, (piece // tile + 2) * lanes), BF16),
        [odd],
        [message],
        "merge",
    )
    message = lax.all_to_all(message, "seq_0", 0, 0)
    context = whole(
        finish_kernel,
        jax.ShapeDtypeStruct((tile, piece // tile * lanes), BF16),
        [bound],
        [message],
        "finish",
    )
    context = spread(spread(context, "seq_0"), "seq_1")
    context = lax.all_gather(context, "seq_2")
    out = whole(
        project_kernel,
        jax.ShapeDtypeStruct((columns, step_count, query_rows), BF16),
        [],
        [context, w_output.T],
        "project",
        [pltpu.VMEM((2, width, lanes), F32)],
    )
    return out.transpose(1, 2, 0)


def solution(mesh):
    finer = Mesh(
        mesh.devices.reshape(mesh.shape["grp"], 16, 4, 2), ("grp", "seq_0", "seq_1", "seq_2")
    )
    return jax.shard_map(
        local,
        mesh=finer,
        in_specs=(
            P("grp", SEQ, None),
            P(None, "grp", None),
            P(None, SEQ),
            P(),
            P(None, SEQ),
            P(),
            P("grp", None),
            P(None, "grp"),
        ),
        out_specs=P(None, "grp", SEQ),
        check_vma=False,
    )
```

```python
import functools
import math

import jax
import jax.numpy as jnp
from jax import lax
from jax.experimental import pallas as pl
from jax.experimental.pallas import tpu as pltpu
from jax.sharding import Mesh
from jax.sharding import PartitionSpec as P

SEQ = ("seq_0", "seq_1", "seq_2")
BF16 = jnp.bfloat16
F32 = jnp.float32
SLAB = 32
PEAK_ROWS = 3
STAT_ROWS = 5
PAIRS = 2
AHEAD = 3
LOG2E = math.log2(math.e)


def split_rows(x, count):
    rows = []
    for _ in range(count):
        part = x.astype(BF16).astype(F32)
        rows.append(part)
        x = x - part
    return rows


def stat_rows(peak, total):
    return split_rows(peak, PEAK_ROWS) + split_rows(total, STAT_ROWS - PEAK_ROWS)


def floor_div(x, n):
    return (x * (2**19 // n + 1)) >> 19


def pair_queries(pair, gathered_ref, rows, columns):
    near, held, _ = gathered_ref.shape
    held -= 16
    window = 48
    span = near * columns
    first = jnp.minimum((pair * rows // span) * columns // 16, (held - window) // 16)
    start = pl.multiple_of(first * 16, 16)
    pieces = [gathered_ref[at, pl.ds(start, window), :] for at in range(near)]
    shape = (rows, near * window)
    at = pair * rows + lax.broadcasted_iota(jnp.int32, (rows, 128), 0)
    far = floor_div(at, span)
    rest = at - far * span
    owner = floor_div(rest, columns)
    column = rest - owner * columns
    source = owner * window + far * columns + column - first * 16
    source = jnp.concatenate([source] * (near * window // 128), axis=1)
    picked = (lax.broadcasted_iota(jnp.int32, shape, 1) == source).astype(F32).astype(BF16)
    queries = jnp.dot(picked, jnp.concatenate(pieces, axis=0), preferred_element_type=F32)
    return queries.astype(BF16)


def attend_kernel(
    lengths_ref,
    slope_ref,
    core_ref,
    gathered_ref,
    k_ref,
    vt_ref,
    dist_ref,
    mine_ref,
    theirs_ref,
    msg_ref,
    stat_ref,
    query_ref,
    *,
    frame_count,
    chunks,
    columns,
    head_size,
):
    step, last = pl.program_id(0), pl.num_programs(0) - 1
    lanes = 2 * head_size
    pairs = k_ref.shape[1] // lanes
    tokens = gathered_ref.shape[2]
    half = tokens // 2
    scale = 1.0 / math.sqrt(head_size)

    def find_queries(step_at, slot):
        for pair in range(pairs):
            query_ref[slot, pair] = pair_queries(
                step_at * pairs + pair, gathered_ref, lanes, columns
            )

    @pl.when(step == 0)
    def _():
        find_queries(0, 0)

    row = lax.broadcasted_iota(jnp.int32, (frame_count, lanes), 0)
    lane = lax.broadcasted_iota(jnp.int32, (frame_count, lanes), 1)
    invalid = [
        jnp.where(jnp.logical_and(row >= lengths_ref[block], lane == 0), 1.0, 0.0).astype(BF16)
        for block in range(2)
    ]
    floor_row = lax.broadcasted_iota(jnp.int32, (lanes, tokens), 0)
    floor = jnp.where(floor_row == 0, -1e30, 0.0).astype(BF16)
    ones = jnp.ones((16, frame_count), BF16)
    zeros = jnp.zeros((head_size, tokens), BF16)
    zeros_half = jnp.zeros((head_size, half), BF16)

    units = [(pair, part) for pair in range(pairs) for part in range(3)]

    def score(pair, part):
        block = 1 if part == 0 else 0
        keys = k_ref[block * frame_count : (block + 1) * frame_count, pair * lanes : (pair + 1) * lanes]
        first = query_ref[step % 2, pair, :head_size, :]
        second = query_ref[step % 2, pair, head_size:, :]
        if part == 0:
            rows = [
                jnp.concatenate([first[:, half:], zeros_half], axis=1),
                jnp.concatenate([zeros_half, second[:, half:]], axis=1),
            ]
        else:
            rows = [first, zeros] if part == 1 else [zeros, second]
        return jnp.dot(
            jnp.concatenate([keys, invalid[block]], axis=1),
            jnp.concatenate(rows + [floor], axis=0),
            preferred_element_type=F32,
        )

    def weigh(pair, part, scores):
        peak = jnp.max(scores, axis=0, keepdims=True)
        weights = jnp.exp2((scores - peak) * (scale * LOG2E)).astype(BF16)
        top = pair * lanes
        if part == 0:
            values = vt_ref[top : top + lanes, frame_count:]
        else:
            start = top + (part - 1) * head_size
            values = vt_ref[start : start + head_size, :frame_count]
        values = jnp.concatenate([values, ones], axis=0)
        return peak * scale, jnp.dot(values, weights, preferred_element_type=F32)

    def emit(pair, side, new, old):
        head = (step * pairs + pair) * 2 + side
        (new_peak, new_sum), (old_peak, old_sum) = new, old
        slope = slope_ref[head]
        late = slice(side * half, (side + 1) * half)
        old_peak = old_peak - slope * dist_ref[0:1, :]
        late_peak = new_peak[:, late] - slope * dist_ref[1:2, half:]
        top = jnp.maximum(old_peak[:, half:], late_peak)
        old_factor = jnp.exp(old_peak[:, half:] - top)
        new_factor = jnp.exp(late_peak - top)
        old_total = old_sum[head_size : head_size + 1, :]
        new_total = new_sum[lanes : lanes + 1, late]
        second = (
            old_sum[:head_size, half:] * old_factor
            + new_sum[side * head_size : (side + 1) * head_size, late] * new_factor
        )
        context = jnp.concatenate([old_sum[:head_size, :half], second], axis=1)
        for part in range(head_size // SLAB):
            slab = head * (head_size // SLAB) + part
            chunk_slabs = (msg_ref.shape[2] - 8) // SLAB
            chunk = slab // chunk_slabs
            place = pl.multiple_of((slab % chunk_slabs) * SLAB, SLAB)
            msg_ref[(chunk + core_ref[0]) % 2, chunk // 2, pl.ds(place, SLAB), :] = context[
                part * SLAB : (part + 1) * SLAB, :
            ]
        stat_ref[head, 0:1, :] = jnp.concatenate([old_peak[:, :half], top], axis=1)
        stat_ref[head, 1:2, :] = jnp.concatenate(
            [old_total[:, :half], old_total[:, half:] * old_factor + new_total * new_factor], axis=1
        )

    ahead = [score(*units[at]) for at in range(AHEAD)]
    done = {}
    for at, (pair, part) in enumerate(units):
        if at + AHEAD < len(units):
            ahead.append(score(*units[at + AHEAD]))
        if at == 1:
            find_queries(jnp.minimum(step + 1, last), 1 - step % 2)
        done[part] = weigh(pair, part, ahead[at])
        ahead[at] = None
        if part > 0:
            emit(pair, part - 1, done[0], done[part])

    @pl.when(step == last)
    def _():
        chunk_rows = msg_ref.shape[2] - 8
        for chunk in range(chunks):
            first = chunk * chunk_rows // head_size
            rows = [stat_ref[head, 0:2, :] for head in range(first, first + 3)]
            rows.append(jnp.zeros_like(rows[0]))
            msg_ref[(chunk + core_ref[0]) % 2, chunk // 2, chunk_rows:, :] = jnp.concatenate(
                rows, axis=0
            )
        mine_ref[...] = msg_ref[0]
        theirs_ref[...] = msg_ref[1]


def attend(lengths, slope, core, gathered, keys, values_t, dist, frame_count, columns):
    near, _, tokens = gathered.shape
    rows, width = keys.shape
    head_count = slope.shape[0]
    head_size = width // head_count
    step_rows = PAIRS * 2 * head_size
    part = (near // 2, width // near + 8, tokens)
    keys, values_t = (pltpu.with_memory_space_constraint(x, pltpu.HBM) for x in (keys, values_t))
    return pl.pallas_call(
        functools.partial(
            attend_kernel,
            frame_count=frame_count,
            chunks=near,
            columns=columns,
            head_size=head_size,
        ),
        grid=(width // step_rows,),
        in_specs=[
            pl.BlockSpec(memory_space=pltpu.SMEM),
            pl.BlockSpec(memory_space=pltpu.SMEM),
            pl.BlockSpec(memory_space=pltpu.SMEM),
            pl.BlockSpec(gathered.shape, lambda p: (0, 0, 0)),
            pl.BlockSpec((rows, step_rows), lambda p: (0, p)),
            pl.BlockSpec((step_rows, rows), lambda p: (p, 0)),
            pl.BlockSpec(dist.shape, lambda p: (0, 0)),
        ],
        out_specs=[pl.BlockSpec(part, lambda p: (0, 0, 0))] * 2,
        out_shape=[jax.ShapeDtypeStruct(part, F32)] * 2,
        scratch_shapes=[
            pltpu.VMEM((2, *part), F32),
            pltpu.VMEM((head_count, 8, tokens), F32),
            pltpu.VMEM((2, PAIRS, 2 * head_size, tokens), BF16),
        ],
        compiler_params=pltpu.CompilerParams(vmem_limit_bytes=40 << 20),
        name="attend",
    )(lengths, slope, core, gathered, keys, values_t, dist)


def slab_value(values, slab, odd):
    even_slot, odd_slot = slab // 2, (slab + 1) // 2
    if even_slot == odd_slot:
        return values[even_slot]
    return jnp.where(odd, values[odd_slot], values[even_slot])


def join_kernel(odd_ref, mine_ref, theirs_ref, out_ref):
    chunks, rows, tokens = mine_ref.shape
    chunk_rows = rows - 8
    odd = odd_ref[0] == 1
    for chunk in range(chunks):
        own, other, stats = [], [], []
        for slot in range(3):
            at = chunk_rows + 2 * slot
            peak, total = mine_ref[chunk, at : at + 1, :], mine_ref[chunk, at + 1 : at + 2, :]
            peak_two = theirs_ref[chunk, at : at + 1, :]
            total_two = theirs_ref[chunk, at + 1 : at + 2, :]
            top = jnp.maximum(peak, peak_two)
            own.append(jnp.exp(peak - top))
            other.append(jnp.exp(peak_two - top))
            stats += stat_rows(top, total * own[slot] + total_two * other[slot])
        for slab in range(chunk_rows // SLAB):
            cut = slice(slab * SLAB, (slab + 1) * SLAB)
            joined = mine_ref[chunk, cut, :] * slab_value(own, slab, odd)
            joined = joined + theirs_ref[chunk, cut, :] * slab_value(other, slab, odd)
            out_ref[chunk, cut, :] = joined.astype(BF16)
        stats.append(jnp.zeros_like(stats[0]))
        out_ref[chunk, chunk_rows:, :] = jnp.concatenate(stats, axis=0).astype(BF16)


def merge_kernel(odd_ref, in_ref, out_ref):
    sources, rows, tokens = in_ref.shape
    chunk_rows = rows - 16
    stats = [in_ref[:, chunk_rows + r, :].astype(F32) for r in range(3 * STAT_ROWS)]
    tops, totals, factors = [], [], []
    for slot in range(3):
        at = slot * STAT_ROWS
        peak = (stats[at] + stats[at + 1]) + stats[at + 2]
        top = jnp.max(peak, axis=0, keepdims=True)
        factor = jnp.exp(peak - top)
        total = jnp.sum(factor * (stats[at + 3] + stats[at + 4]), axis=0, keepdims=True)
        rounded = total.astype(BF16).astype(F32)
        tops.append(top)
        totals.append(rounded)
        factors.append(factor * (rounded / total))
    odd = odd_ref[0] == 1
    slabs, slab_stats = [], []
    for slab in range(chunk_rows // SLAB):
        factor = slab_value(factors, slab, odd)
        merged = None
        for source in range(sources):
            part = in_ref[source, slab * SLAB : (slab + 1) * SLAB, :].astype(F32)
            part = part * factor[source : source + 1, :]
            merged = part if merged is None else merged + part
        slabs.append(merged)
        rows = split_rows(slab_value(tops, slab, odd), PEAK_ROWS)
        slab_stats.append(jnp.concatenate(rows + [slab_value(totals, slab, odd)], axis=0))
    merged = jnp.concatenate(slabs, axis=0)
    targets, tile, width = out_ref.shape
    lanes = tokens // 2
    pieces = targets // 2
    piece = chunk_rows // pieces
    for target in range(targets):
        side, at = target // pieces, (target % pieces) * piece
        cut = slice(side * lanes, (side + 1) * lanes)
        tiles = [merged[at + r : at + r + tile, cut] for r in range(0, piece, tile)]
        tiles += [slab_stats[at // SLAB][:, cut], slab_stats[(at + piece - 1) // SLAB][:, cut]]
        out_ref[target] = jnp.concatenate(tiles, axis=1).astype(BF16)


def finish_kernel(bound_ref, in_ref, out_ref):
    tile, width = out_ref.shape
    lanes = (in_ref.shape[2] - width) // 2
    factors, totals = [], []
    for head in range(2):
        cut = slice(width + head * lanes, width + (head + 1) * lanes)
        stats = in_ref[:, :, cut].astype(F32)
        peak = (stats[:, 0:1, :] + stats[:, 1:2, :]) + stats[:, 2:3, :]
        factor = jnp.exp(peak - jnp.max(peak, axis=0, keepdims=True))
        factors.append(factor)
        totals.append(jnp.sum(factor * stats[:, 3:4, :], axis=0))
    for at in range(width // lanes):
        cut = slice(at * lanes, (at + 1) * lanes)
        first = at * tile < bound_ref[0]
        factor = jnp.where(first, factors[0], factors[1])
        context = jnp.sum(in_ref[:, :, cut].astype(F32) * factor, axis=0)
        out_ref[:, cut] = (context / jnp.where(first, totals[0], totals[1])).astype(BF16)


def ask_kernel(w_ref, dec_ref, out_ref):
    columns, tokens = w_ref.shape[0], dec_ref.shape[0]
    lanes = tokens // 2
    queries = lax.dot_general(
        w_ref[...], dec_ref[...], (((1,), (1,)), ((), ())), preferred_element_type=F32
    )
    sides = [queries[:, :lanes], queries[:, lanes:]]
    tiles = [side[at : at + 4] for side in sides for at in range(0, columns - 2, 4)]
    tiles.append(jnp.concatenate([side[columns - 2 :] for side in sides], axis=0))
    tiles = jnp.concatenate(tiles, axis=1).astype(BF16)
    for target in range(out_ref.shape[0]):
        out_ref[target] = tiles


def columns_kernel(w_ref, out_ref):
    chunks, rows, lanes = out_ref.shape
    columns, width = w_ref.shape
    part = width // chunks
    weights = w_ref[...].astype(F32)
    for chunk in range(chunks):
        own = weights[:, chunk * part : (chunk + 1) * part]
        own = jnp.concatenate([own, jnp.zeros((columns, lanes - part), F32)], axis=1)
        own = jnp.concatenate([own, jnp.zeros((rows - columns, lanes), F32)], axis=0)
        out_ref[chunk] = own.astype(BF16)


def pack_kernel(tiles_ref, w_ref, out_ref, rows_ref, *, columns):
    targets = tiles_ref.shape[0]
    tokens = out_ref.shape[2]
    lanes = tokens // 2
    whole_tiles = (columns - 2) // 4
    for source in range(targets):
        held = tiles_ref[source].astype(F32)
        tiles = [held[:, at * lanes : (at + 1) * lanes] for at in range(2 * whole_tiles + 1)]
        top = source * columns
        for side in range(2):
            cut = slice(side * lanes, (side + 1) * lanes)
            for at in range(whole_tiles):
                rows_ref[top + 4 * at : top + 4 * at + 4, cut] = tiles[side * whole_tiles + at]
            rows_ref[top + columns - 2 : top + columns, cut] = tiles[-1][2 * side : 2 * side + 2]
    rows = rows_ref[...].astype(BF16)
    for target in range(out_ref.shape[0]):
        out_ref[target, : rows.shape[0], :] = rows
        out_ref[target, rows.shape[0] :, :] = w_ref[target]


def project_kernel(ctx_ref, w_ref, out_ref, rows_ref):
    targets, tile, width = ctx_ref.shape
    part, tokens = rows_ref.shape
    lanes = tokens // 2
    pieces = targets // 2
    piece = width // lanes * tile
    for target in range(targets):
        held = ctx_ref[target].astype(F32)
        side = target // pieces
        for at in range(width // lanes):
            start = (target % pieces) * piece + at * tile
            rows_ref[start : start + tile, side * lanes : (side + 1) * lanes] = held[
                :, at * lanes : (at + 1) * lanes
            ]
    sources, rows, _ = w_ref.shape
    weights = jnp.concatenate([w_ref[source, :, :part] for source in range(sources)], axis=0)
    out = jnp.dot(weights, rows_ref[...].astype(BF16), preferred_element_type=F32)
    for source in range(sources):
        out_ref[source] = out[source * rows : (source + 1) * rows]


def sum_kernel(in_ref, out_ref):
    columns, sides, lanes = out_ref.shape
    total = jnp.sum(in_ref[...], axis=0)
    for side in range(sides):
        out_ref[:, side, :] = total[:columns, side * lanes : (side + 1) * lanes].astype(BF16)


def whole(kernel, out_shape, scalars, arrays, name, scratch=()):
    return pl.pallas_call(
        kernel,
        in_specs=[pl.BlockSpec(memory_space=pltpu.SMEM)] * len(scalars)
        + [pl.BlockSpec(memory_space=pltpu.VMEM)] * len(arrays),
        out_specs=pl.BlockSpec(memory_space=pltpu.VMEM),
        out_shape=out_shape,
        scratch_shapes=scratch,
        compiler_params=pltpu.CompilerParams(vmem_limit_bytes=32 << 20),
        name=name,
    )(*scalars, *arrays)


def spread(x, axis):
    copies = jnp.broadcast_to(x[None], (lax.axis_size(axis), *x.shape))
    copies = lax.optimization_barrier(copies)
    return lax.all_to_all(copies, axis, 0, 0)


def local(frames, dec_states, w_query, w_keyval, w_output, head_slope, lengths, positions):
    devices = lax.axis_size(SEQ)
    own_index = lax.axis_index(SEQ)
    across, beside, cores = (lax.axis_size(axis) for axis in SEQ)
    step_count, frame_count, width = frames.shape
    query_rows = dec_states.shape[1]
    tokens = step_count * query_rows
    columns = w_query.shape[1]
    near = beside * cores

    lanes = tokens // 2
    tile = 4
    part = width // near
    asked = whole(
        ask_kernel,
        jax.ShapeDtypeStruct((across, tile, columns * tokens // tile), BF16),
        [],
        [
            pltpu.with_memory_space_constraint(x, pltpu.HBM)
            for x in (w_query.T, dec_states.reshape(tokens, width))
        ],
        "ask",
    )
    out_columns = whole(
        columns_kernel,
        jax.ShapeDtypeStruct((near, 16, tokens), BF16),
        [],
        [w_output.T],
        "columns",
    )
    queries = lax.all_to_all(asked, "seq_0", 0, 0)
    queries, late_frames = lax.optimization_barrier((queries, frames))
    queries = whole(
        functools.partial(pack_kernel, columns=columns),
        pltpu.HBM((near, part + 16, tokens), BF16),
        [],
        [queries, out_columns],
        "pack",
        [pltpu.VMEM((part, tokens), F32)],
    )
    queries = lax.all_to_all(queries, SEQ[1:], 0, 0)

    frame_rows = frames.reshape(step_count * frame_count, width)
    keys = jnp.dot(frame_rows, w_keyval[:, :width], preferred_element_type=F32).astype(BF16)
    late_rows = late_frames.reshape(step_count * frame_count, width)
    values_t = lax.dot_general(
        w_keyval[:, width:], late_rows, (((0,), (1,)), ((), ())), preferred_element_type=F32
    ).astype(BF16)

    slot_place = ((own_index + 1) % devices).astype(F32)
    apart = jnp.abs(positions.astype(F32) - slot_place) / devices
    age = jnp.arange(step_count, dtype=F32)[:, None]
    dist = jnp.stack([(apart + age).reshape(tokens), apart.reshape(tokens)])
    dist = jnp.pad(dist, ((0, 6), (0, 0)))
    own_lengths = lax.dynamic_slice(lengths, (0, own_index), (step_count, 1)).reshape(step_count)

    odd = (lax.axis_index(("seq_1", "seq_2")) % 2).astype(jnp.int32).reshape(1)
    piece = 2 * width // devices
    at = (lax.axis_index("seq_0") % (across // 2)) * piece
    bound = (SLAB - at % SLAB).astype(jnp.int32).reshape(1)
    core = lax.axis_index("seq_2").astype(jnp.int32).reshape(1)
    queries, odd, bound, core, dist, own_lengths = lax.optimization_barrier(
        (queries, odd, bound, core, dist, own_lengths)
    )
    mine, theirs = attend(
        own_lengths, head_slope, core, queries, keys, values_t, dist, frame_count, columns
    )
    theirs, asked_columns = lax.optimization_barrier((theirs, queries))
    out_columns = asked_columns[:, part:, :]
    theirs = lax.ppermute(theirs, "seq_2", [(at, cores - 1 - at) for at in range(cores)])
    theirs, out_columns = lax.optimization_barrier((theirs, out_columns))
    message = whole(
        join_kernel,
        jax.ShapeDtypeStruct((beside, width // near + 16, tokens), BF16),
        [odd],
        [mine, theirs],
        "join",
    )
    message = lax.all_to_all(message, "seq_1", 0, 0)
    message = whole(
        merge_kernel,
        jax.ShapeDtypeStruct((across, tile, (piece // tile + 2) * lanes), BF16),
        [odd],
        [message],
        "merge",
    )
    message = lax.all_to_all(message, "seq_0", 0, 0)
    context = whole(
        finish_kernel,
        jax.ShapeDtypeStruct((tile, piece // tile * lanes), BF16),
        [bound],
        [message],
        "finish",
    )
    context = spread(context, "seq_0")
    partial = whole(
        project_kernel,
        jax.ShapeDtypeStruct((near, 16, tokens), F32),
        [],
        [context, out_columns],
        "project",
        [pltpu.VMEM((part, tokens), F32)],
    )
    partial = lax.all_to_all(partial, SEQ[1:], 0, 0)
    out = whole(
        sum_kernel,
        jax.ShapeDtypeStruct((columns, step_count, query_rows), BF16),
        [],
        [partial],
        "sum",
    )
    return out.transpose(1, 2, 0)


def solution(mesh):
    finer = Mesh(
        mesh.devices.reshape(mesh.shape["grp"], 16, 4, 2), ("grp", "seq_0", "seq_1", "seq_2")
    )
    return jax.shard_map(
        local,
        mesh=finer,
        in_specs=(
            P("grp", SEQ, None),
            P(None, "grp", None),
            P(None, SEQ),
            P(),
            P(None, SEQ),
            P(),
            P("grp", None),
            P(None, "grp"),
        ),
        out_specs=P(None, "grp", SEQ),
        check_vma=False,
    )
```

```python
import functools
import math

import jax
import jax.numpy as jnp
from jax import lax
from jax.experimental import pallas as pl
from jax.experimental.pallas import tpu as pltpu
from jax.sharding import Mesh
from jax.sharding import PartitionSpec as P

SEQ = ("seq_0", "seq_1", "seq_2")
BF16 = jnp.bfloat16
F32 = jnp.float32
SLAB = 32
PEAK_ROWS = 3
STAT_ROWS = 5
PAIRS = 2
AHEAD = 3
KEY_COLUMNS = 256
LOG2E = math.log2(math.e)


def split_rows(x, count):
    rows = []
    for _ in range(count):
        part = x.astype(BF16).astype(F32)
        rows.append(part)
        x = x - part
    return rows


def stat_rows(peak, total):
    return split_rows(peak, PEAK_ROWS) + split_rows(total, STAT_ROWS - PEAK_ROWS)


def floor_div(x, n):
    return (x * (2**19 // n + 1)) >> 19


def pair_queries(pair, gathered_ref, rows, columns):
    near, held, _ = gathered_ref.shape
    held -= 16
    window = 48
    span = near * columns
    first = jnp.minimum((pair * rows // span) * columns // 16, (held - window) // 16)
    start = pl.multiple_of(first * 16, 16)
    pieces = [gathered_ref[at, pl.ds(start, window), :] for at in range(near)]
    shape = (rows, near * window)
    at = pair * rows + lax.broadcasted_iota(jnp.int32, (rows, 128), 0)
    far = floor_div(at, span)
    rest = at - far * span
    owner = floor_div(rest, columns)
    column = rest - owner * columns
    source = owner * window + far * columns + column - first * 16
    source = jnp.concatenate([source] * (near * window // 128), axis=1)
    picked = (lax.broadcasted_iota(jnp.int32, shape, 1) == source).astype(F32).astype(BF16)
    queries = jnp.dot(picked, jnp.concatenate(pieces, axis=0), preferred_element_type=F32)
    return queries.astype(BF16)


def attend_kernel(
    lengths_ref,
    slope_ref,
    core_ref,
    index_ref,
    gathered_ref,
    k_ref,
    vt_ref,
    dist_ref,
    mine_ref,
    theirs_ref,
    msg_ref,
    stat_ref,
    query_ref,
    *,
    frame_count,
    chunks,
    columns,
    head_size,
):
    step, last = pl.program_id(0), pl.num_programs(0) - 1
    lanes = 2 * head_size
    pairs = k_ref.shape[1] // lanes
    tokens = gathered_ref.shape[2]
    half = tokens // 2
    scale = 1.0 / math.sqrt(head_size)

    def find_queries(step_at, slot):
        for pair in range(pairs):
            query_ref[slot, pair] = pair_queries(
                step_at * pairs + pair, gathered_ref, lanes, columns
            )

    @pl.when(step == 0)
    def _():
        find_queries(0, 0)

    row = lax.broadcasted_iota(jnp.int32, (frame_count, lanes), 0)
    lane = lax.broadcasted_iota(jnp.int32, (frame_count, lanes), 1)
    invalid = [
        jnp.where(jnp.logical_and(row >= lengths_ref[block, index_ref[0]], lane == 0), 1.0, 0.0).astype(BF16)
        for block in range(2)
    ]
    floor_row = lax.broadcasted_iota(jnp.int32, (lanes, tokens), 0)
    floor = jnp.where(floor_row == 0, -1e30, 0.0).astype(BF16)
    ones = jnp.ones((16, frame_count), BF16)
    zeros = jnp.zeros((head_size, tokens), BF16)
    zeros_half = jnp.zeros((head_size, half), BF16)

    units = [(pair, part) for pair in range(pairs) for part in range(3)]

    def score(pair, part):
        block = 1 if part == 0 else 0
        keys = k_ref[block * frame_count : (block + 1) * frame_count, pair * lanes : (pair + 1) * lanes]
        first = query_ref[step % 2, pair, :head_size, :]
        second = query_ref[step % 2, pair, head_size:, :]
        if part == 0:
            rows = [
                jnp.concatenate([first[:, half:], zeros_half], axis=1),
                jnp.concatenate([zeros_half, second[:, half:]], axis=1),
            ]
        else:
            rows = [first, zeros] if part == 1 else [zeros, second]
        return jnp.dot(
            jnp.concatenate([keys, invalid[block]], axis=1),
            jnp.concatenate(rows + [floor], axis=0),
            preferred_element_type=F32,
        )

    def weigh(pair, part, scores):
        peak = jnp.max(scores, axis=0, keepdims=True)
        weights = jnp.exp2((scores - peak) * (scale * LOG2E)).astype(BF16)
        top = pair * lanes
        if part == 0:
            values = vt_ref[top : top + lanes, frame_count:]
        else:
            start = top + (part - 1) * head_size
            values = vt_ref[start : start + head_size, :frame_count]
        values = jnp.concatenate([values, ones], axis=0)
        return peak * scale, jnp.dot(values, weights, preferred_element_type=F32)

    def emit(pair, side, new, old):
        head = (step * pairs + pair) * 2 + side
        (new_peak, new_sum), (old_peak, old_sum) = new, old
        slope = slope_ref[head]
        late = slice(side * half, (side + 1) * half)
        old_peak = old_peak - slope * dist_ref[0:1, :]
        late_peak = new_peak[:, late] - slope * dist_ref[1:2, half:]
        top = jnp.maximum(old_peak[:, half:], late_peak)
        old_factor = jnp.exp(old_peak[:, half:] - top)
        new_factor = jnp.exp(late_peak - top)
        old_total = old_sum[head_size : head_size + 1, :]
        new_total = new_sum[lanes : lanes + 1, late]
        second = (
            old_sum[:head_size, half:] * old_factor
            + new_sum[side * head_size : (side + 1) * head_size, late] * new_factor
        )
        context = jnp.concatenate([old_sum[:head_size, :half], second], axis=1)
        for part in range(head_size // SLAB):
            slab = head * (head_size // SLAB) + part
            chunk_slabs = (msg_ref.shape[2] - 8) // SLAB
            chunk = slab // chunk_slabs
            place = pl.multiple_of((slab % chunk_slabs) * SLAB, SLAB)
            msg_ref[(chunk + core_ref[0]) % 2, chunk // 2, pl.ds(place, SLAB), :] = context[
                part * SLAB : (part + 1) * SLAB, :
            ]
        stat_ref[head, 0:1, :] = jnp.concatenate([old_peak[:, :half], top], axis=1)
        stat_ref[head, 1:2, :] = jnp.concatenate(
            [old_total[:, :half], old_total[:, half:] * old_factor + new_total * new_factor], axis=1
        )

    ahead = [score(*units[at]) for at in range(AHEAD)]
    done = {}
    for at, (pair, part) in enumerate(units):
        if at + AHEAD < len(units):
            ahead.append(score(*units[at + AHEAD]))
        if at == 1:
            find_queries(jnp.minimum(step + 1, last), 1 - step % 2)
        done[part] = weigh(pair, part, ahead[at])
        ahead[at] = None
        if part > 0:
            emit(pair, part - 1, done[0], done[part])

    @pl.when(step == last)
    def _():
        chunk_rows = msg_ref.shape[2] - 8
        for chunk in range(chunks):
            first = chunk * chunk_rows // head_size
            rows = [stat_ref[head, 0:2, :] for head in range(first, first + 3)]
            rows.append(jnp.zeros_like(rows[0]))
            msg_ref[(chunk + core_ref[0]) % 2, chunk // 2, chunk_rows:, :] = jnp.concatenate(
                rows, axis=0
            )
        mine_ref[...] = msg_ref[0]
        theirs_ref[...] = msg_ref[1]


def attend(lengths, slope, core, index, gathered, keys, values_t, dist, frame_count, columns):
    near, _, tokens = gathered.shape
    rows, width = keys.shape
    head_count = slope.shape[0]
    head_size = width // head_count
    step_rows = PAIRS * 2 * head_size
    part = (near // 2, width // near + 8, tokens)
    keys, values_t = (pltpu.with_memory_space_constraint(x, pltpu.HBM) for x in (keys, values_t))
    return pl.pallas_call(
        functools.partial(
            attend_kernel,
            frame_count=frame_count,
            chunks=near,
            columns=columns,
            head_size=head_size,
        ),
        grid=(width // step_rows,),
        in_specs=[
            pl.BlockSpec(memory_space=pltpu.SMEM),
            pl.BlockSpec(memory_space=pltpu.SMEM),
            pl.BlockSpec(memory_space=pltpu.SMEM),
            pl.BlockSpec(memory_space=pltpu.SMEM),
            pl.BlockSpec(gathered.shape, lambda p: (0, 0, 0)),
            pl.BlockSpec((rows, step_rows), lambda p: (0, p)),
            pl.BlockSpec((step_rows, rows), lambda p: (p, 0)),
            pl.BlockSpec(dist.shape, lambda p: (0, 0)),
        ],
        out_specs=[pl.BlockSpec(part, lambda p: (0, 0, 0))] * 2,
        out_shape=[jax.ShapeDtypeStruct(part, F32)] * 2,
        scratch_shapes=[
            pltpu.VMEM((2, *part), F32),
            pltpu.VMEM((head_count, 8, tokens), F32),
            pltpu.VMEM((2, PAIRS, 2 * head_size, tokens), BF16),
        ],
        compiler_params=pltpu.CompilerParams(vmem_limit_bytes=40 << 20),
        name="attend",
    )(lengths, slope, core, index, gathered, keys, values_t, dist)


def slab_value(values, slab, odd):
    even_slot, odd_slot = slab // 2, (slab + 1) // 2
    if even_slot == odd_slot:
        return values[even_slot]
    return jnp.where(odd, values[odd_slot], values[even_slot])


def join_kernel(odd_ref, mine_ref, theirs_ref, out_ref):
    chunks, rows, tokens = mine_ref.shape
    chunk_rows = rows - 8
    odd = odd_ref[0] == 1
    for chunk in range(chunks):
        own, other, stats = [], [], []
        for slot in range(3):
            at = chunk_rows + 2 * slot
            peak, total = mine_ref[chunk, at : at + 1, :], mine_ref[chunk, at + 1 : at + 2, :]
            peak_two = theirs_ref[chunk, at : at + 1, :]
            total_two = theirs_ref[chunk, at + 1 : at + 2, :]
            top = jnp.maximum(peak, peak_two)
            own.append(jnp.exp(peak - top))
            other.append(jnp.exp(peak_two - top))
            stats += stat_rows(top, total * own[slot] + total_two * other[slot])
        for slab in range(chunk_rows // SLAB):
            cut = slice(slab * SLAB, (slab + 1) * SLAB)
            joined = mine_ref[chunk, cut, :] * slab_value(own, slab, odd)
            joined = joined + theirs_ref[chunk, cut, :] * slab_value(other, slab, odd)
            out_ref[chunk, cut, :] = joined.astype(BF16)
        stats.append(jnp.zeros_like(stats[0]))
        out_ref[chunk, chunk_rows:, :] = jnp.concatenate(stats, axis=0).astype(BF16)


def merge_kernel(odd_ref, in_ref, out_ref):
    sources, rows, tokens = in_ref.shape
    chunk_rows = rows - 16
    stats = [in_ref[:, chunk_rows + r, :].astype(F32) for r in range(3 * STAT_ROWS)]
    tops, totals, factors = [], [], []
    for slot in range(3):
        at = slot * STAT_ROWS
        peak = (stats[at] + stats[at + 1]) + stats[at + 2]
        top = jnp.max(peak, axis=0, keepdims=True)
        factor = jnp.exp(peak - top)
        total = jnp.sum(factor * (stats[at + 3] + stats[at + 4]), axis=0, keepdims=True)
        rounded = total.astype(BF16).astype(F32)
        tops.append(top)
        totals.append(rounded)
        factors.append(factor * (rounded / total))
    odd = odd_ref[0] == 1
    slabs, slab_stats = [], []
    for slab in range(chunk_rows // SLAB):
        factor = slab_value(factors, slab, odd)
        merged = None
        for source in range(sources):
            part = in_ref[source, slab * SLAB : (slab + 1) * SLAB, :].astype(F32)
            part = part * factor[source : source + 1, :]
            merged = part if merged is None else merged + part
        slabs.append(merged)
        rows = split_rows(slab_value(tops, slab, odd), PEAK_ROWS)
        slab_stats.append(jnp.concatenate(rows + [slab_value(totals, slab, odd)], axis=0))
    merged = jnp.concatenate(slabs, axis=0)
    targets, tile, width = out_ref.shape
    lanes = tokens // 2
    pieces = targets // 2
    piece = chunk_rows // pieces
    for target in range(targets):
        side, at = target // pieces, (target % pieces) * piece
        cut = slice(side * lanes, (side + 1) * lanes)
        tiles = [merged[at + r : at + r + tile, cut] for r in range(0, piece, tile)]
        tiles += [slab_stats[at // SLAB][:, cut], slab_stats[(at + piece - 1) // SLAB][:, cut]]
        out_ref[target] = jnp.concatenate(tiles, axis=1).astype(BF16)


def finish_kernel(bound_ref, in_ref, out_ref):
    tile, width = out_ref.shape
    lanes = (in_ref.shape[2] - width) // 2
    factors, totals = [], []
    for head in range(2):
        cut = slice(width + head * lanes, width + (head + 1) * lanes)
        stats = in_ref[:, :, cut].astype(F32)
        peak = (stats[:, 0:1, :] + stats[:, 1:2, :]) + stats[:, 2:3, :]
        factor = jnp.exp(peak - jnp.max(peak, axis=0, keepdims=True))
        factors.append(factor)
        totals.append(jnp.sum(factor * stats[:, 3:4, :], axis=0))
    for at in range(width // lanes):
        cut = slice(at * lanes, (at + 1) * lanes)
        first = at * tile < bound_ref[0]
        factor = jnp.where(first, factors[0], factors[1])
        context = jnp.sum(in_ref[:, :, cut].astype(F32) * factor, axis=0)
        out_ref[:, cut] = (context / jnp.where(first, totals[0], totals[1])).astype(BF16)


def ask_kernel(w_ref, dec_ref, out_ref):
    columns, tokens = w_ref.shape[0], dec_ref.shape[0]
    lanes = tokens // 2
    queries = lax.dot_general(
        w_ref[...], dec_ref[...], (((1,), (1,)), ((), ())), preferred_element_type=F32
    )
    sides = [queries[:, :lanes], queries[:, lanes:]]
    tiles = [side[at : at + 4] for side in sides for at in range(0, columns - 2, 4)]
    tiles.append(jnp.concatenate([side[columns - 2 :] for side in sides], axis=0))
    tiles = jnp.concatenate(tiles, axis=1).astype(BF16)
    for target in range(out_ref.shape[0]):
        out_ref[target] = tiles


def project_keys_kernel(frames_ref, w_ref, out_ref):
    out_ref[...] = jnp.dot(frames_ref[...], w_ref[...], preferred_element_type=F32).astype(BF16)


def columns_kernel(w_ref, out_ref):
    chunks, rows, lanes = out_ref.shape
    columns, width = w_ref.shape
    part = width // chunks
    weights = w_ref[...].astype(F32)
    for chunk in range(chunks):
        own = weights[:, chunk * part : (chunk + 1) * part]
        own = jnp.concatenate([own, jnp.zeros((columns, lanes - part), F32)], axis=1)
        own = jnp.concatenate([own, jnp.zeros((rows - columns, lanes), F32)], axis=0)
        out_ref[chunk] = own.astype(BF16)


def pack_kernel(tiles_ref, w_ref, out_ref, rows_ref, *, columns):
    targets = tiles_ref.shape[0]
    tokens = out_ref.shape[2]
    lanes = tokens // 2
    whole_tiles = (columns - 2) // 4
    for source in range(targets):
        held = tiles_ref[source].astype(F32)
        tiles = [held[:, at * lanes : (at + 1) * lanes] for at in range(2 * whole_tiles + 1)]
        top = source * columns
        for side in range(2):
            cut = slice(side * lanes, (side + 1) * lanes)
            for at in range(whole_tiles):
                rows_ref[top + 4 * at : top + 4 * at + 4, cut] = tiles[side * whole_tiles + at]
            rows_ref[top + columns - 2 : top + columns, cut] = tiles[-1][2 * side : 2 * side + 2]
    rows = rows_ref[...].astype(BF16)
    for target in range(out_ref.shape[0]):
        out_ref[target, : rows.shape[0], :] = rows
        out_ref[target, rows.shape[0] :, :] = w_ref[target]


def project_kernel(ctx_ref, w_ref, out_ref, rows_ref):
    targets, tile, width = ctx_ref.shape
    part, tokens = rows_ref.shape
    lanes = tokens // 2
    pieces = targets // 2
    piece = width // lanes * tile
    for target in range(targets):
        held = ctx_ref[target].astype(F32)
        side = target // pieces
        for at in range(width // lanes):
            start = (target % pieces) * piece + at * tile
            rows_ref[start : start + tile, side * lanes : (side + 1) * lanes] = held[
                :, at * lanes : (at + 1) * lanes
            ]
    sources, rows, _ = w_ref.shape
    weights = jnp.concatenate([w_ref[source, :, :part] for source in range(sources)], axis=0)
    out = jnp.dot(weights, rows_ref[...].astype(BF16), preferred_element_type=F32)
    for source in range(sources):
        out_ref[source] = out[source * rows : (source + 1) * rows]


def sum_kernel(in_ref, out_ref):
    columns, sides, lanes = out_ref.shape
    total = jnp.sum(in_ref[...], axis=0)
    for side in range(sides):
        out_ref[:, side, :] = total[:columns, side * lanes : (side + 1) * lanes].astype(BF16)


def whole(kernel, out_shape, scalars, arrays, name, scratch=()):
    return pl.pallas_call(
        kernel,
        in_specs=[pl.BlockSpec(memory_space=pltpu.SMEM)] * len(scalars)
        + [pl.BlockSpec(memory_space=pltpu.VMEM)] * len(arrays),
        out_specs=pl.BlockSpec(memory_space=pltpu.VMEM),
        out_shape=out_shape,
        scratch_shapes=scratch,
        compiler_params=pltpu.CompilerParams(vmem_limit_bytes=32 << 20),
        name=name,
    )(*scalars, *arrays)


def spread(x, axis):
    copies = jnp.broadcast_to(x[None], (lax.axis_size(axis), *x.shape))
    copies = lax.optimization_barrier(copies)
    return lax.all_to_all(copies, axis, 0, 0)


def local(frames, dec_states, w_query, w_keyval, w_output, head_slope, lengths, positions):
    devices = lax.axis_size(SEQ)
    own_index = lax.axis_index(SEQ)
    across, beside, cores = (lax.axis_size(axis) for axis in SEQ)
    step_count, frame_count, width = frames.shape
    query_rows = dec_states.shape[1]
    tokens = step_count * query_rows
    columns = w_query.shape[1]
    near = beside * cores

    lanes = tokens // 2
    tile = 4
    part = width // near
    asked = whole(
        ask_kernel,
        jax.ShapeDtypeStruct((across, tile, columns * tokens // tile), BF16),
        [],
        [
            pltpu.with_memory_space_constraint(x, pltpu.HBM)
            for x in (w_query.T, dec_states.reshape(tokens, width))
        ],
        "ask",
    )
    out_columns = whole(
        columns_kernel,
        jax.ShapeDtypeStruct((near, 16, tokens), BF16),
        [],
        [w_output.T],
        "columns",
    )
    queries = lax.all_to_all(asked, "seq_0", 0, 0)
    queries, late_frames = lax.optimization_barrier((queries, frames))
    queries = whole(
        functools.partial(pack_kernel, columns=columns),
        pltpu.HBM((near, part + 16, tokens), BF16),
        [],
        [queries, out_columns],
        "pack",
        [pltpu.VMEM((part, tokens), F32)],
    )
    queries = lax.all_to_all(queries, SEQ[1:], 0, 0)

    frame_rows = frames.reshape(step_count * frame_count, width)
    keys = pl.pallas_call(
        project_keys_kernel,
        grid=(width // KEY_COLUMNS,),
        in_specs=[
            pl.BlockSpec((step_count * frame_count, width), lambda p: (0, 0)),
            pl.BlockSpec((width, KEY_COLUMNS), lambda p: (0, p)),
        ],
        out_specs=pl.BlockSpec((step_count * frame_count, KEY_COLUMNS), lambda p: (0, p)),
        out_shape=pltpu.HBM((step_count * frame_count, width), BF16),
        compiler_params=pltpu.CompilerParams(vmem_limit_bytes=32 << 20),
        cost_estimate=pl.CostEstimate(
            flops=2 * step_count * frame_count * width * width,
            transcendentals=0,
            bytes_accessed=2 * width * (2 * step_count * frame_count + width),
        ),
        name="keys",
    )(frame_rows, pltpu.with_memory_space_constraint(w_keyval, pltpu.HBM))
    late_rows = late_frames.reshape(step_count * frame_count, width)
    values_t = lax.dot_general(
        w_keyval[:, width:], late_rows, (((0,), (1,)), ((), ())), preferred_element_type=F32
    ).astype(BF16)

    slot_place = ((own_index + 1) % devices).astype(F32)
    apart = jnp.abs(positions.astype(F32) - slot_place) / devices
    age = jnp.arange(step_count, dtype=F32)[:, None]
    dist = jnp.stack([(apart + age).reshape(tokens), apart.reshape(tokens)])
    dist = jnp.pad(dist, ((0, 6), (0, 0)))
    index = own_index.astype(jnp.int32).reshape(1)

    odd = (lax.axis_index(("seq_1", "seq_2")) % 2).astype(jnp.int32).reshape(1)
    piece = 2 * width // devices
    at = (lax.axis_index("seq_0") % (across // 2)) * piece
    bound = (SLAB - at % SLAB).astype(jnp.int32).reshape(1)
    core = lax.axis_index("seq_2").astype(jnp.int32).reshape(1)
    queries, odd, bound, core, dist, index = lax.optimization_barrier(
        (queries, odd, bound, core, dist, index)
    )
    mine, theirs = attend(
        lengths, head_slope, core, index, queries, keys, values_t, dist, frame_count, columns
    )
    theirs, asked_columns = lax.optimization_barrier((theirs, queries))
    out_columns = asked_columns[:, part:, :]
    theirs = lax.ppermute(theirs, "seq_2", [(at, cores - 1 - at) for at in range(cores)])
    theirs, out_columns = lax.optimization_barrier((theirs, out_columns))
    message = whole(
        join_kernel,
        jax.ShapeDtypeStruct((beside, width // near + 16, tokens), BF16),
        [odd],
        [mine, theirs],
        "join",
    )
    message = lax.all_to_all(message, "seq_1", 0, 0)
    message = whole(
        merge_kernel,
        jax.ShapeDtypeStruct((across, tile, (piece // tile + 2) * lanes), BF16),
        [odd],
        [message],
        "merge",
    )
    message = lax.all_to_all(message, "seq_0", 0, 0)
    context = whole(
        finish_kernel,
        jax.ShapeDtypeStruct((tile, piece // tile * lanes), BF16),
        [bound],
        [message],
        "finish",
    )
    context = spread(context, "seq_0")
    partial = whole(
        project_kernel,
        jax.ShapeDtypeStruct((near, 16, tokens), F32),
        [],
        [context, out_columns],
        "project",
        [pltpu.VMEM((part, tokens), F32)],
    )
    partial = lax.all_to_all(partial, SEQ[1:], 0, 0)
    out = whole(
        sum_kernel,
        jax.ShapeDtypeStruct((columns, step_count, query_rows), BF16),
        [],
        [partial],
        "sum",
    )
    return out.transpose(1, 2, 0)


def solution(mesh):
    finer = Mesh(
        mesh.devices.reshape(mesh.shape["grp"], 16, 4, 2), ("grp", "seq_0", "seq_1", "seq_2")
    )
    return jax.shard_map(
        local,
        mesh=finer,
        in_specs=(
            P("grp", SEQ, None),
            P(None, "grp", None),
            P(None, SEQ),
            P(),
            P(None, SEQ),
            P(),
            P("grp", None),
            P(None, "grp"),
        ),
        out_specs=P(None, "grp", SEQ),
        check_vma=False,
    )
```
